256 devices in a mesh: row: 8 (over x, y_lo), col: 32 (over z, y_hi, core).
Axes of the slice: x: 4, y: 4 (y_hi: 2, y_lo: 2; y = y_hi * 2 + y_lo), z: 8, core: 2. Of those that a mesh axis runs over, the one named last changes fastest.
Arguments:
- grad_out: bfloat16 [2048, 8192], P('col', 'row'), may hold values from -6 to 6
- weight: bfloat16 [28672, 8192], P('col', 'row'), may hold values from -0.0625 to 0.0625
Outputs:
- grad_in: bfloat16 [2048, 28672], P('row', 'col')
The draws below stay inside these ranges and needn't reach their ends.
All inputs are finite; a program needn't handle non-finite values.
Results may differ from the reference program's by a relative error of at most 0.001.
Values may be sent and summed in bfloat16 or wider, within the bound.
A program may use at most 64 MiB of HBM per device.

```python
import jax
import jax.numpy as jnp
from jax import lax

D = 8192
FF = 28672
TOKENS = 2048


def with_spikes(array, key, source, target, parts, factor):
    def block_of(axis_at):
        return (jnp.arange(array.shape[axis_at]) // (array.shape[axis_at] // parts)).reshape((-1,) + (1,) * (array.ndim - 1 - axis_at))

    near = jax.random.permutation(key, parts)[block_of(target)]
    second = (block_of(target) + parts // 2) % parts
    return jnp.where((block_of(source) == near) | (block_of(source) == second), factor * array, array)


def shard_levels(rng, dims, split, low, top_value):
    def one(dim, blocks):
        heights = jax.random.uniform(jax.random.fold_in(jax.random.fold_in(rng, 6), dim), (blocks,), jnp.float32, low / len(split), top_value / len(split))
        return jnp.repeat(jnp.exp(heights), dims[dim] // blocks).reshape((-1,) + (1,) * (len(dims) - dim - 1))

    factor_of = one(*split[0])
    for cut in split[1:]:
        factor_of = factor_of * one(*cut)
    return factor_of


def centred(own_key, dims, spread, reach, cuts=(), dtype=jnp.bfloat16):
    values = jax.random.normal(own_key, dims, jnp.float32) * spread
    if len(cuts) > 0:
        values = shard_levels(own_key, dims, cuts, -0.22, 0.18) * values
    return jnp.clip(values, min=-reach, max=reach).astype(dtype)


def bell_draw_with(stream_key, dims, spread, bound, split, heavy, held_as=jnp.bfloat16):
    array = spread * jax.random.normal(stream_key, dims, jnp.float32)
    if split:
        array = array * shard_levels(stream_key, dims, split, -0.22, 0.18)
    return jnp.clip(with_spikes(array, jax.random.fold_in(stream_key, 3), *heavy), -bound, bound).astype(held_as)


def setup_inputs(seed: int = 0) -> dict:
    key_list = jax.random.split(jax.random.key(seed), 3)
    grad_out = bell_draw_with(key_list[0], (TOKENS, D), 1.0, 6.0, ((0, 32), (1, 8)), (1, 0, 32, 2.75))
    weight = centred(key_list[1], (FF, D), D ** -0.5, 0.0625, ((0, 32), (1, 8)))
    return {"grad_out": grad_out, "weight": weight}


def reference(grad_out, weight):
    blocks = weight.reshape(8, FF // 8, D)

    def one_block(block):
        return jnp.dot(grad_out, block.T, preferred_element_type=jnp.float32).astype(jnp.bfloat16)

    result = lax.map(one_block, blocks)
    return jnp.transpose(result, (1, 0, 2)).reshape(TOKENS, FF)
```

```python
import jax
import jax.numpy as jnp
from jax import lax
from jax.experimental import pallas as pl
from jax.experimental.pallas import tpu as pltpu
from jax.sharding import PartitionSpec as P

MESH = pl.DeviceIdType.MESH
CH = 128
L_REL = (0, 1, 1, 0)
H_REL = (0, 0, 1, 1)
NT = (((1,), (1,)), ((), ()))


def kernel(
    g_ref, w_ref, o_ref, gbuf, wn, cbuf, relay, farin, nearin,
    s1s, s1r, zs, zr, ps, pr, ws, wr, fs, fr, ds, dr, rs, rr,
):
    n_ch = w_ref.shape[0] // CH
    tb, feat = g_ref.shape
    blk = 4 * tb
    half = blk // 2
    row = lax.axis_index("row")
    col = lax.axis_index("col")
    x = lax.div(row, 2)
    lo = lax.rem(row, 2)
    z = lax.div(col, 4)
    hi = lax.rem(lax.div(col, 2), 2)
    c = lax.rem(col, 2)
    is_src = lax.rem(z, 2) == lo

    def dev(x=x, lo=lo, z=z, hi=hi, c=c):
        return (x * 2 + lo, z * 4 + hi * 2 + c)

    zn = (lax.rem(z + 1, 8), lax.rem(z + 7, 8))
    xn = (lax.rem(x + 1, 4), lax.rem(x + 3, 4))
    partner = dev(c=1 - c)
    z_dev = (dev(z=zn[0]), dev(z=zn[1]))
    x_dev = (dev(x=xn[0]), dev(x=xn[1]))
    w_dev = dev(lo=1 - lo)
    h_dev = dev(hi=1 - hi)
    wh_dev = dev(lo=1 - lo, hi=1 - hi)

    barrier = pltpu.get_barrier_semaphore()
    peers = (partner, *z_dev, *x_dev, w_dev, h_dev, wh_dev)
    for peer in peers:
        pl.semaphore_signal(barrier, inc=1, device_id=peer, device_id_type=MESH)
    pl.semaphore_wait(barrier, len(peers))

    def rc(src, dst, ss, sr, to):
        return pltpu.make_async_remote_copy(
            src_ref=src, dst_ref=dst, send_sem=ss, recv_sem=sr, device_id=to, device_id_type=MESH
        )

    def block(slot, k, core):
        h = hi if H_REL[k] == 0 else 1 - hi
        at = pl.multiple_of(slot * blk + (h * 2 + core) * tb, tb)
        return gbuf.at[L_REL[k], pl.ds(at, tb), :]

    def place(slot, l, h, core):
        at = pl.multiple_of(slot * blk + (h * 2 + core) * tb, tb)
        return gbuf.at[l, pl.ds(at, tb), :]

    def slot_of(shift):
        return lax.div(lax.rem(z + shift, 8), 2)

    s0 = lax.div(z, 2)

    def pidx(d, r, k):
        return 4 + d * 8 + r * 4 + k

    @pl.when(is_src)
    def _():
        own = place(s0, 0, hi, c)
        rc(g_ref, place(s0, 0, hi, c), s1s.at[0], s1r.at[2], h_dev).start()
        for d in range(2):
            rc(g_ref, own, zs.at[d, 0, 0], zr.at[d, 0, 0], z_dev[d]).start()
        rc(g_ref, own, ps.at[0], pr.at[0], partner).start()

    @pl.when(jnp.logical_not(is_src))
    def _():
        rc(g_ref, place(s0, 1, hi, c), s1s.at[0], s1r.at[0], w_dev).start()
        rc(g_ref, place(s0, 1, hi, c), s1s.at[1], s1r.at[1], wh_dev).start()

    def w_copy(j):
        at = pl.ds(pl.multiple_of(j * CH, CH), CH)
        return rc(w_ref.at[at, :], wn.at[at, :], ws.at[j], wr.at[j], w_dev)

    for j in range(n_ch):
        w_copy(j).start()

    def relay_to(slot, k, d, out_r, send_r):
        b = block(slot, k, c)
        rc(b, b, zs.at[d, send_r, k], zr.at[d, out_r, k], z_dev[d]).start()

    def share(slot, k, i):
        b = block(slot, k, c)
        rc(b, b, ps.at[i], pr.at[i], partner).start()

    def arrived(slot, k, d, r):
        b = block(slot, k, c)
        rc(b, b, zs.at[d, r, k], zr.at[d, r, k], z_dev[d]).wait_recv()

    @pl.when(is_src)
    def _():
        gbuf[0, pl.ds(pl.multiple_of(s0 * blk + (hi * 2 + c) * tb, tb), tb), :] = g_ref[...]
        for k in range(1, 4):
            b = block(s0, k, c)
            rc(b, b, s1s.at[0], s1r.at[k - 1], h_dev).wait_recv()
            for d in range(2):
                relay_to(s0, k, d, 0, 0)
            share(s0, k, k)
        near = (slot_of(6), slot_of(2))
        for k in range(4):
            for d in range(2):
                arrived(near[d], k, d, 0)
                relay_to(near[d], k, d, 1, 1)
                share(near[d], k, pidx(d, 0, k))
        opp = slot_of(4)
        for i in range(2):
            for d in range(2):
                k = d * 2 + i
                arrived(opp, k, d, 1)
                share(opp, k, pidx(d, 1, k))
        for k in range(4):
            b = block(s0, k, 1 - c)
            rc(b, b, ps.at[k], pr.at[k], partner).wait_recv()
            for d in range(2):
                b = block(near[d], k, 1 - c)
                i = pidx(d, 0, k)
                rc(b, b, ps.at[i], pr.at[i], partner).wait_recv()
        for d in range(2):
            for i in range(2):
                k = d * 2 + i
                b = block(opp, k, 1 - c)
                i = pidx(d, 1, k)
                rc(b, b, ps.at[i], pr.at[i], partner).wait_recv()

    @pl.when(jnp.logical_not(is_src))
    def _():
        near = (slot_of(7), slot_of(1))
        far = (slot_of(5), slot_of(3))
        for k in range(4):
            for d in range(2):
                arrived(near[d], k, d, 0)
                relay_to(near[d], k, d, 0, 0)
                share(near[d], k, pidx(d, 0, k))
        for k in (0, 2, 1, 3):
            for d in range(2):
                arrived(far[d], k, d, 1)
                if k // 2 == d:
                    relay_to(far[d], k, d, 1, 1)
                share(far[d], k, pidx(d, 1, k))
        for r, slots in ((0, near), (1, far)):
            for k in range(4):
                for d in range(2):
                    b = block(slots[d], k, 1 - c)
                    i = pidx(d, r, k)
                    rc(b, b, ps.at[i], pr.at[i], partner).wait_recv()

    far_slot = lax.rem(x + 2, 4)

    def far_copy(j, d):
        src = cbuf.at[j, pl.ds(pl.multiple_of(far_slot * blk + d * half, half), half), :]
        return rc(src, farin.at[d, j], fs.at[d, j], fr.at[d, j], x_dev[d])

    def direct_copy(j, d):
        at = (1 - d) * half
        src = cbuf.at[j, pl.ds(pl.multiple_of(xn[d] * blk + at, half), half), :]
        return rc(src, nearin.at[d, j, pl.ds(at, half), :], ds.at[d, j], dr.at[d, j], x_dev[d])

    def relay_copy(j, d):
        dst = nearin.at[d, j, pl.ds(d * half, half), :]
        return rc(relay.at[d, j], dst, rs.at[d, j], rr.at[d, j], x_dev[d])

    def step(j, _):
        @pl.when(j < n_ch)
        def _():
            w_copy(j).wait_recv()
            at = pl.ds(pl.multiple_of(j * CH, CH), CH)

            def compute(slot):
                rows = pl.ds(pl.multiple_of(slot * blk, blk), blk)
                total = lax.dot_general(gbuf[0, rows, :], w_ref[at, :], NT, preferred_element_type=jnp.float32)
                total += lax.dot_general(gbuf[1, rows, :], wn[at, :], NT, preferred_element_type=jnp.float32)
                cbuf[j, rows, :] = total

            compute(far_slot)
            for d in range(2):
                far_copy(j, d).start()
            for d in range(2):
                compute(xn[d])
                direct_copy(j, d).start()
            compute(x)

        @pl.when(jnp.logical_and(j >= 1, j <= n_ch))
        def _():
            i = j - 1
            for d in range(2):
                far_copy(i, d).wait_recv()
                rows = pl.ds(pl.multiple_of(xn[d] * blk + d * half, half), half)
                relay[d, i] = cbuf[i, rows, :] + farin[d, i]
                relay_copy(i, d).start()

        @pl.when(j >= 2)
        def _():
            i = j - 2
            for d in range(2):
                direct_copy(i, d).wait_recv()
                relay_copy(i, d).wait_recv()
            rows = pl.ds(pl.multiple_of(x * blk, blk), blk)
            total = cbuf[i, rows, :] + nearin[0, i] + nearin[1, i]
            o_ref[:, pl.ds(pl.multiple_of(i * CH, CH), CH)] = total.astype(o_ref.dtype)

        return 0

    lax.fori_loop(0, n_ch + 2, step, 0)

    def drain(j, _):
        w_copy(j).wait_send()
        for d in range(2):
            far_copy(j, d).wait_send()
            direct_copy(j, d).wait_send()
            relay_copy(j, d).wait_send()
        return 0

    lax.fori_loop(0, n_ch, drain, 0)

    def sent(sem):
        rc(g_ref, g_ref, sem, sem, partner).wait_send()

    sent(s1s.at[0])
    for d in range(2):
        for k in range(4):
            sent(zs.at[d, 0, k])
            sent(ps.at[pidx(d, 0, k)])
            if k // 2 == d:
                sent(zs.at[d, 1, k])
                sent(ps.at[pidx(d, 1, k)])

    @pl.when(is_src)
    def _():
        for k in range(4):
            sent(ps.at[k])
        for d in range(2):
            for k in range(4):
                if k // 2 != d:
                    sent(zs.at[d, 1, k])

    @pl.when(jnp.logical_not(is_src))
    def _():
        sent(s1s.at[1])
        for d in range(2):
            for k in range(4):
                if k // 2 != d:
                    sent(ps.at[pidx(d, 1, k)])


def local(grad_out, weight):
    tb, feat = grad_out.shape
    hidden = weight.shape[0]
    n_ch = hidden // CH
    blk = 4 * tb
    dma = pltpu.SemaphoreType.DMA
    vmem = pl.BlockSpec(memory_space=pltpu.VMEM)
    return pl.pallas_call(
        kernel,
        out_shape=jax.ShapeDtypeStruct((blk, hidden), jnp.bfloat16),
        in_specs=[vmem, vmem],
        out_specs=vmem,
        scratch_shapes=[
            pltpu.VMEM((2, 4 * blk, feat), jnp.bfloat16),
            pltpu.VMEM((hidden, feat), jnp.bfloat16),
            pltpu.VMEM((n_ch, 4 * blk, CH), jnp.float32),
            pltpu.VMEM((2, n_ch, blk // 2, CH), jnp.float32),
            pltpu.VMEM((2, n_ch, blk // 2, CH), jnp.float32),
            pltpu.VMEM((2, n_ch, blk, CH), jnp.float32),
            dma((2,)), dma((3,)),
            dma((2, 2, 4)), dma((2, 2, 4)),
            dma((20,)), dma((20,)),
            dma((n_ch,)), dma((n_ch,)),
            dma((2, n_ch)), dma((2, n_ch)),
            dma((2, n_ch)), dma((2, n_ch)),
            dma((2, n_ch)), dma((2, n_ch)),
        ],
        compiler_params=pltpu.CompilerParams(
            collective_id=0, has_side_effects=True, vmem_limit_bytes=48 * 1024 * 1024
        ),
    )(grad_out, weight)


def solution(mesh):
    spec = P("col", "row")
    return jax.shard_map(local, mesh=mesh, in_specs=(spec, spec), out_specs=P("row", "col"), check_vma=False)
```

```python
import jax
import jax.numpy as jnp
from jax import lax
from jax.experimental import pallas as pl
from jax.experimental.pallas import tpu as pltpu
from jax.sharding import PartitionSpec as P

MESH = pl.DeviceIdType.MESH
CH = 128
ORDER = (0, 2, 1, 3)
NT = (((1,), (1,)), ((), ()))


def kernel(
    g_hbm, w_hbm, o_ref, g_ref, w_ref, gbuf, wn, cbuf, relay, farin, nearin,
    ls, s1s, s1r, zs, zr, ps, pr, ws, wr, fs, fr, ds, dr, rs, rr,
):
    n_ch = w_ref.shape[0] // CH
    tb, feat = g_ref.shape
    blk = 4 * tb
    half = blk // 2
    n_items = 2 * n_ch
    row = lax.axis_index("row")
    col = lax.axis_index("col")
    x = lax.div(row, 2)
    lo = lax.rem(row, 2)
    z = lax.div(col, 4)
    hi = lax.rem(lax.div(col, 2), 2)
    c = lax.rem(col, 2)
    is_src = lax.rem(z, 2) == lo
    not_src = jnp.logical_not(is_src)

    def dev(x=x, lo=lo, z=z, hi=hi, c=c):
        return (x * 2 + lo, z * 4 + hi * 2 + c)

    zn = (lax.rem(z + 1, 8), lax.rem(z + 7, 8))
    xn = (lax.rem(x + 1, 4), lax.rem(x + 3, 4))
    partner = dev(c=1 - c)
    z_dev = (dev(z=zn[0]), dev(z=zn[1]))
    x_dev = (dev(x=xn[0]), dev(x=xn[1]))
    w_dev = dev(lo=1 - lo)
    h_dev = dev(hi=1 - hi)
    wh_dev = dev(lo=1 - lo, hi=1 - hi)

    barrier = pltpu.get_barrier_semaphore()
    peers = (partner, *z_dev, *x_dev, w_dev, h_dev, wh_dev)
    for peer in peers:
        pl.semaphore_signal(barrier, inc=1, device_id=peer, device_id_type=MESH)
    g_in = pltpu.make_async_copy(g_hbm, g_ref, ls.at[0])
    w_in = pltpu.make_async_copy(w_hbm, w_ref, ls.at[1])
    g_in.start()
    w_in.start()
    g_in.wait()
    w_in.wait()
    pl.semaphore_wait(barrier, len(peers))

    def rc(src, dst, ss, sr, to):
        return pltpu.make_async_remote_copy(
            src_ref=src, dst_ref=dst, send_sem=ss, recv_sem=sr, device_id=to, device_id_type=MESH
        )

    def place(slot, l, h, core):
        at = pl.multiple_of(slot * blk + (h * 2 + core) * tb, tb)
        return gbuf.at[l, pl.ds(at, tb), :]

    def block(slot, k, core):
        return place(slot, lax.rem(lax.div(k + 1, 2), 2), lax.rem(hi + lax.div(k, 2), 2), core)

    def slot_of(shift):
        return lax.div(lax.rem(z + shift, 8), 2)

    s0 = lax.div(z, 2)

    def pidx(d, r, k):
        return 4 + d * 8 + r * 4 + k

    @pl.when(is_src)
    def _():
        own = place(s0, 0, hi, c)
        rc(g_ref, own, s1s.at[0], s1r.at[2], h_dev).start()
        for d in range(2):
            rc(g_ref, own, zs.at[d, 0, 0], zr.at[d, 0, 0], z_dev[d]).start()
        rc(g_ref, own, ps.at[0], pr.at[0], partner).start()

    @pl.when(not_src)
    def _():
        rc(g_ref, place(s0, 1, hi, c), s1s.at[0], s1r.at[0], w_dev).start()
        rc(g_ref, place(s0, 1, hi, c), s1s.at[1], s1r.at[1], wh_dev).start()

    def w_copy(j):
        at = pl.ds(pl.multiple_of(j * CH, CH), CH)
        return rc(w_ref.at[at, :], wn.at[at, :], ws.at[j], wr.at[j], w_dev)

    for j in range(n_ch):
        w_copy(j).start()

    def relay_to(slot, k, d, out_r, send_r):
        b = block(slot, k, c)
        rc(b, b, zs.at[d, send_r, k], zr.at[d, out_r, k], z_dev[d]).start()

    def share(slot, k, i):
        b = block(slot, k, c)
        rc(b, b, ps.at[i], pr.at[i], partner).start()

    def arrived(slot, k, d, r):
        b = block(slot, k, c)
        rc(b, b, zs.at[d, r, k], zr.at[d, r, k], z_dev[d]).wait_recv()

    def shared(slot, k, i):
        b = block(slot, k, 1 - c)
        rc(b, b, ps.at[i], pr.at[i], partner).wait_recv()

    src_near = (slot_of(6), slot_of(2))
    opp = slot_of(4)
    mid_near = (slot_of(7), slot_of(1))
    mid_far = (slot_of(5), slot_of(3))
    early = (jnp.where(is_src, s0, mid_near[0]), jnp.where(is_src, src_near[1], mid_near[1]))
    late = (jnp.where(is_src, src_near[0], mid_far[0]), jnp.where(is_src, opp, mid_far[1]))

    @pl.when(is_src)
    def _():
        gbuf[0, pl.ds(pl.multiple_of(s0 * blk + (hi * 2 + c) * tb, tb), tb), :] = g_ref[...]
        for k in (2, 1, 3):
            b = block(s0, k, c)
            rc(b, b, s1s.at[0], s1r.at[k - 1], h_dev).wait_recv()
            for d in range(2):
                relay_to(s0, k, d, 0, 0)
            share(s0, k, k)
        for k in ORDER:
            for d in range(2):
                arrived(src_near[d], k, d, 0)
                relay_to(src_near[d], k, d, 1, 1)
                share(src_near[d], k, pidx(d, 0, k))
        for k in range(4):
            shared(s0, k, k)
            shared(src_near[1], k, pidx(1, 0, k))

    @pl.when(not_src)
    def _():
        for k in ORDER:
            for d in range(2):
                arrived(mid_near[d], k, d, 0)
                relay_to(mid_near[d], k, d, 0, 0)
                share(mid_near[d], k, pidx(d, 0, k))
        for k in range(4):
            for d in range(2):
                shared(mid_near[d], k, pidx(d, 0, k))

    def gather_step(t):
        @pl.when(jnp.logical_and(not_src, t < 4))
        def _():
            k = 2 * lax.rem(t, 2) + lax.div(t, 2)
            for d in range(2):
                arrived(mid_far[d], k, d, 1)

                @pl.when(lax.rem(t, 2) == d)
                def _():
                    relay_to(mid_far[d], k, d, 1, 1)

                share(mid_far[d], k, pidx(d, 1, k))

        @pl.when(jnp.logical_and(is_src, jnp.logical_and(t >= 2, t < 4)))
        def _():
            for d in range(2):
                k = d * 2 + t - 2
                arrived(opp, k, d, 1)
                share(opp, k, pidx(d, 1, k))

        @pl.when(jnp.logical_and(not_src, t == 4))
        def _():
            for k in range(4):
                for d in range(2):
                    shared(mid_far[d], k, pidx(d, 1, k))

        @pl.when(jnp.logical_and(is_src, t == 4))
        def _():
            for k in range(4):
                shared(src_near[0], k, pidx(0, 0, k))
                shared(opp, k, pidx(k // 2, 1, k))

    def group_of(t):
        u = jnp.maximum(t, 0)
        tail = u >= 8
        e = jnp.where(tail, lax.rem(u, 2), lax.div(u, 4))
        j = jnp.where(tail, lax.div(u, 2), lax.rem(u, 4))
        pair = tuple(jnp.where(e == 0, early[i], late[i]) for i in range(2))
        return e, j, pair

    def inside(slot, pair):
        return jnp.logical_or(slot == pair[0], slot == pair[1])

    far_slot = lax.rem(x + 2, 4)

    def far_copy(j, d):
        src = cbuf.at[j, pl.ds(pl.multiple_of(far_slot * blk + d * half, half), half), :]
        return rc(src, farin.at[d, j], fs.at[d, j], fr.at[d, j], x_dev[d])

    def direct_copy(j, d):
        at = (1 - d) * half
        src = cbuf.at[j, pl.ds(pl.multiple_of(xn[d] * blk + at, half), half), :]
        return rc(src, nearin.at[d, j, pl.ds(at, half), :], ds.at[d, j], dr.at[d, j], x_dev[d])

    def relay_copy(j, d):
        dst = nearin.at[d, j, pl.ds(d * half, half), :]
        return rc(relay.at[d, j], dst, rs.at[d, j], rr.at[d, j], x_dev[d])

    def relay_step(t):
        _, j, pair = group_of(t)
        live = jnp.logical_and(t >= 0, t < n_items)
        for d in range(2):
            @pl.when(jnp.logical_and(live, inside(xn[d], pair)))
            def _():
                far_copy(j, d).wait_recv()
                rows = pl.ds(pl.multiple_of(xn[d] * blk + d * half, half), half)
                relay[d, j] = cbuf[j, rows, :] + farin[d, j]
                relay_copy(j, d).start()

    def final_step(t):
        _, j, pair = group_of(t)

        @pl.when(jnp.logical_and(t >= 0, inside(x, pair)))
        def _():
            for d in range(2):
                direct_copy(j, d).wait_recv()
                relay_copy(j, d).wait_recv()
            rows = pl.ds(pl.multiple_of(x * blk, blk), blk)
            total = cbuf[j, rows, :] + nearin[0, j] + nearin[1, j]
            o_ref[:, pl.ds(pl.multiple_of(j * CH, CH), CH)] = total.astype(o_ref.dtype)

    def compute_step(t):
        e, j, pair = group_of(t)

        @pl.when(t < n_items)
        def _():
            @pl.when(e == 0)
            def _():
                w_copy(j).wait_recv()

            at = pl.ds(pl.multiple_of(j * CH, CH), CH)
            for slot in pair:
                rows = pl.ds(pl.multiple_of(slot * blk, blk), blk)
                total = lax.dot_general(gbuf[0, rows, :], w_ref[at, :], NT, preferred_element_type=jnp.float32)
                total += lax.dot_general(gbuf[1, rows, :], wn[at, :], NT, preferred_element_type=jnp.float32)
                cbuf[j, rows, :] = total

                @pl.when(slot == far_slot)
                def _():
                    for d in range(2):
                        far_copy(j, d).start()

                for d in range(2):
                    @pl.when(slot == xn[d])
                    def _():
                        direct_copy(j, d).start()

    def step(t, _):
        gather_step(t)
        relay_step(t - 2)
        final_step(t - 4)
        compute_step(t)
        return 0

    lax.fori_loop(0, n_items + 4, step, 0)

    def drain(j, _):
        w_copy(j).wait_send()
        for d in range(2):
            far_copy(j, d).wait_send()
            direct_copy(j, d).wait_send()
            relay_copy(j, d).wait_send()
        return 0

    lax.fori_loop(0, n_ch, drain, 0)

    def sent(sem):
        rc(g_ref, g_ref, sem, sem, partner).wait_send()

    sent(s1s.at[0])
    for d in range(2):
        for k in range(4):
            sent(zs.at[d, 0, k])
            sent(ps.at[pidx(d, 0, k)])
            if k // 2 == d:
                sent(zs.at[d, 1, k])
                sent(ps.at[pidx(d, 1, k)])

    @pl.when(is_src)
    def _():
        for k in range(4):
            sent(ps.at[k])
        for d in range(2):
            for k in range(4):
                if k // 2 != d:
                    sent(zs.at[d, 1, k])

    @pl.when(not_src)
    def _():
        sent(s1s.at[1])
        for d in range(2):
            for k in range(4):
                if k // 2 != d:
                    sent(ps.at[pidx(d, 1, k)])


def local(grad_out, weight):
    tb, feat = grad_out.shape
    hidden = weight.shape[0]
    n_ch = hidden // CH
    blk = 4 * tb
    dma = pltpu.SemaphoreType.DMA
    vmem = pl.BlockSpec(memory_space=pltpu.VMEM)
    hbm = pl.BlockSpec(memory_space=pltpu.HBM)
    return pl.pallas_call(
        kernel,
        out_shape=jax.ShapeDtypeStruct((blk, hidden), jnp.bfloat16),
        in_specs=[hbm, hbm],
        out_specs=vmem,
        scratch_shapes=[
            pltpu.VMEM((tb, feat), jnp.bfloat16),
            pltpu.VMEM((hidden, feat), jnp.bfloat16),
            pltpu.VMEM((2, 4 * blk, feat), jnp.bfloat16),
            pltpu.VMEM((hidden, feat), jnp.bfloat16),
            pltpu.VMEM((n_ch, 4 * blk, CH), jnp.float32),
            pltpu.VMEM((2, n_ch, blk // 2, CH), jnp.float32),
            pltpu.VMEM((2, n_ch, blk // 2, CH), jnp.float32),
            pltpu.VMEM((2, n_ch, blk, CH), jnp.float32),
            dma((2,)),
            dma((2,)), dma((3,)),
            dma((2, 2, 4)), dma((2, 2, 4)),
            dma((20,)), dma((20,)),
            dma((n_ch,)), dma((n_ch,)),
            dma((2, n_ch)), dma((2, n_ch)),
            dma((2, n_ch)), dma((2, n_ch)),
            dma((2, n_ch)), dma((2, n_ch)),
        ],
        compiler_params=pltpu.CompilerParams(
            collective_id=0, has_side_effects=True, vmem_limit_bytes=63 * 1024 * 1024
        ),
    )(grad_out, weight)


def solution(mesh):
    spec = P("col", "row")
    return jax.shard_map(local, mesh=mesh, in_specs=(spec, spec), out_specs=P("row", "col"), check_vma=False)
```

```python
import jax
import jax.numpy as jnp
from jax import lax
from jax.experimental import pallas as pl
from jax.experimental.pallas import tpu as pltpu
from jax.sharding import PartitionSpec as P

MESH = pl.DeviceIdType.MESH
CH = 128
ORDER = (0, 1, 3, 2)
SIDE = (0, 1, 1, 0)
SPLIT = 8
LAG = 3
LAST = 6
NT = (((1,), (1,)), ((), ()))


def kernel(
    g_hbm, w_hbm, o_ref, g_ref, w_ref, gbuf, wn, cbuf, relay, farin, nearin,
    ls, s1s, s1r, zs, zr, ps, pr, ws, wr, fs, fr, ds, dr,
):
    n_ch = w_ref.shape[0] // CH
    tb, feat = g_ref.shape
    blk = 4 * tb
    half = blk // 2
    row = lax.axis_index("row")
    col = lax.axis_index("col")
    x = lax.div(row, 2)
    lo = lax.rem(row, 2)
    z = lax.div(col, 4)
    hi = lax.rem(lax.div(col, 2), 2)
    c = lax.rem(col, 2)
    is_src = lax.rem(z, 2) == lo
    not_src = jnp.logical_not(is_src)

    def dev(x=x, lo=lo, z=z, hi=hi, c=c):
        return (x * 2 + lo, z * 4 + hi * 2 + c)

    zn = (lax.rem(z + 1, 8), lax.rem(z + 7, 8))
    xn = (lax.rem(x + 1, 4), lax.rem(x + 3, 4))
    partner = dev(c=1 - c)
    z_dev = (dev(z=zn[0]), dev(z=zn[1]))
    x_dev = (dev(x=xn[0]), dev(x=xn[1]))
    w_dev = dev(lo=1 - lo)
    h_dev = dev(hi=1 - hi)
    wh_dev = dev(lo=1 - lo, hi=1 - hi)

    barrier = pltpu.get_barrier_semaphore()
    peers = (partner, *z_dev, *x_dev, w_dev, h_dev, wh_dev)
    for peer in peers:
        pl.semaphore_signal(barrier, inc=1, device_id=peer, device_id_type=MESH)
    g_in = pltpu.make_async_copy(g_hbm, g_ref, ls.at[0])
    w_in = pltpu.make_async_copy(w_hbm, w_ref, ls.at[1])
    g_in.start()
    w_in.start()
    g_in.wait()
    w_in.wait()
    pl.semaphore_wait(barrier, len(peers))

    def rc(src, dst, ss, sr, to):
        return pltpu.make_async_remote_copy(
            src_ref=src, dst_ref=dst, send_sem=ss, recv_sem=sr, device_id=to, device_id_type=MESH
        )

    def place(slot, l, h, core):
        at = pl.multiple_of(slot * blk + (h * 2 + core) * tb, tb)
        return gbuf.at[l, pl.ds(at, tb), :]

    def side(k):
        return lax.rem(lax.div(k + 1, 2), 2)

    def block(slot, k, core):
        return place(slot, side(k), lax.rem(hi + lax.div(k, 2), 2), core)

    def slot_of(shift):
        return lax.div(lax.rem(z + shift, 8), 2)

    s0 = lax.div(z, 2)

    def pidx(d, r, k):
        return 4 + d * 8 + r * 4 + k

    @pl.when(is_src)
    def _():
        own = place(s0, 0, hi, c)
        rc(g_ref, own, s1s.at[0], s1r.at[2], h_dev).start()
        for d in range(2):
            rc(g_ref, own, zs.at[d, 0, 0], zr.at[d, 0, 0], z_dev[d]).start()
        rc(g_ref, own, ps.at[0], pr.at[0], partner).start()

    @pl.when(not_src)
    def _():
        rc(g_ref, place(s0, 1, hi, c), s1s.at[0], s1r.at[0], w_dev).start()
        rc(g_ref, place(s0, 1, hi, c), s1s.at[1], s1r.at[1], wh_dev).start()

    def w_copy(j):
        at = pl.ds(pl.multiple_of(j * CH, CH), CH)
        return rc(w_ref.at[at, :], wn.at[at, :], ws.at[j], wr.at[j], w_dev)

    for j in range(n_ch):
        w_copy(j).start()

    def relay_to(slot, k, d, out_r, send_r):
        b = block(slot, k, c)
        rc(b, b, zs.at[d, send_r, k], zr.at[d, out_r, k], z_dev[d]).start()

    def share(slot, k, i):
        b = block(slot, k, c)
        rc(b, b, ps.at[i], pr.at[i], partner).start()

    def arrived(slot, k, d, r):
        b = block(slot, k, c)
        rc(b, b, zs.at[d, r, k], zr.at[d, r, k], z_dev[d]).wait_recv()

    def shared(slot, k, i):
        b = block(slot, k, 1 - c)
        rc(b, b, ps.at[i], pr.at[i], partner).wait_recv()

    src_near = (slot_of(6), slot_of(2))
    opp = slot_of(4)
    mid_near = (slot_of(7), slot_of(1))
    mid_far = (slot_of(5), slot_of(3))
    early = (jnp.where(is_src, s0, mid_near[0]), jnp.where(is_src, src_near[1], mid_near[1]))
    late = (jnp.where(is_src, src_near[0], mid_far[0]), jnp.where(is_src, opp, mid_far[1]))

    @pl.when(is_src)
    def _():
        gbuf[0, pl.ds(pl.multiple_of(s0 * blk + (hi * 2 + c) * tb, tb), tb), :] = g_ref[...]
        for k in ORDER[1:]:
            b = block(s0, k, c)
            rc(b, b, s1s.at[0], s1r.at[k - 1], h_dev).wait_recv()
            for d in range(2):
                relay_to(s0, k, d, 0, 0)
            share(s0, k, k)
        for k in ORDER:
            for d in range(2):
                arrived(src_near[d], k, d, 0)
                relay_to(src_near[d], k, d, 1, 1)
                share(src_near[d], k, pidx(d, 0, k))
        for k in range(4):
            shared(s0, k, k)
            shared(src_near[1], k, pidx(1, 0, k))

    @pl.when(not_src)
    def _():
        for k in ORDER:
            for d in range(2):
                arrived(mid_near[d], k, d, 0)
                relay_to(mid_near[d], k, d, 0, 0)
                share(mid_near[d], k, pidx(d, 0, k))
        for k in range(4):
            for d in range(2):
                shared(mid_near[d], k, pidx(d, 0, k))

    def gather_step(t):
        @pl.when(jnp.logical_and(not_src, t < 4))
        def _():
            k = jnp.where(t < 2, t, 5 - t)
            for d in range(2):
                arrived(mid_far[d], k, d, 1)

                @pl.when(side(k) == d)
                def _():
                    relay_to(mid_far[d], k, d, 1, 1)

                share(mid_far[d], k, pidx(d, 1, k))

        @pl.when(jnp.logical_and(is_src, jnp.logical_and(t >= 2, t < 4)))
        def _():
            for d in range(2):
                k = d + (t - 2) * (3 - 2 * d)
                arrived(opp, k, d, 1)
                share(opp, k, pidx(d, 1, k))

        @pl.when(jnp.logical_and(not_src, t == 4))
        def _():
            for k in range(4):
                for d in range(2):
                    shared(mid_far[d], k, pidx(d, 1, k))

        @pl.when(jnp.logical_and(is_src, t == 4))
        def _():
            for k in range(4):
                shared(src_near[0], k, pidx(0, 0, k))
                shared(opp, k, pidx(SIDE[k], 1, k))

    n_items = SPLIT + n_ch - SPLIT // 2
    flush = n_items - 1
    far_slot = lax.rem(x + 2, 4)
    order = (far_slot, xn[0], xn[1], x)

    def group_of(t):
        full = t >= SPLIT
        e = lax.div(t, SPLIT // 2)
        j = jnp.where(full, t - SPLIT // 2, lax.rem(t, SPLIT // 2))
        pair = tuple(jnp.where(full, order[i], jnp.where(e == 0, early[i], late[i])) for i in range(2))
        return full, e, j, pair

    def inside(slot, full, pair):
        return jnp.logical_or(full, jnp.logical_or(slot == pair[0], slot == pair[1]))

    def way(slot, h, full, pair):
        other = pair[0] + pair[1] - slot
        return jnp.where(full, h, jnp.where(lax.rem(slot + 1, 4) == other, 0, 1))

    def rows_of(slot, h):
        return pl.ds(pl.multiple_of(slot * blk + h * half, half), half)

    def far_copy(j, d, h):
        return rc(cbuf.at[j, rows_of(far_slot, h), :], farin.at[d, j, h], fs.at[j, h], fr.at[d, j, h], x_dev[d])

    def near_dst(j, d, h):
        return nearin.at[d, j, pl.ds(h * half, half), :]

    def direct_copy(j, d, h):
        return rc(cbuf.at[j, rows_of(xn[d], h), :], near_dst(j, d, h), ds.at[d, j, h], dr.at[d, j, h], x_dev[d])

    def relay_copy(j, d, h):
        return rc(relay.at[d, j, h], near_dst(j, d, h), ds.at[d, j, h], dr.at[d, j, h], x_dev[d])

    def relay_step(t, _):
        full, _, j, pair = group_of(t)
        for h in range(2):
            for d in range(2):
                @pl.when(jnp.logical_and(inside(xn[d], full, pair), way(xn[d], h, full, pair) == d))
                def _():
                    far_copy(j, d, h).wait_recv()
                    relay[d, j, h] = cbuf[j, rows_of(xn[d], h), :] + farin[d, j, h]
                    relay_copy(j, d, h).start()

        return 0

    def final_step(t, _):
        full, _, j, pair = group_of(t)

        @pl.when(inside(x, full, pair))
        def _():
            for h in range(2):
                for d in range(2):
                    direct_copy(j, d, h).wait_recv()
            rows = pl.ds(pl.multiple_of(x * blk, blk), blk)
            total = cbuf[j, rows, :] + nearin[0, j] + nearin[1, j]
            o_ref[:, pl.ds(pl.multiple_of(j * CH, CH), CH)] = total.astype(o_ref.dtype)

        return 0

    def compute_step(t):
        full, e, j, pair = group_of(t)

        @pl.when(jnp.logical_or(full, e == 0))
        def _():
            w_copy(j).wait_recv()

        at = pl.ds(pl.multiple_of(j * CH, CH), CH)

        def one(i, _):
            slot = jnp.where(i < 2, jnp.where(i == 0, pair[0], pair[1]), jnp.where(i == 2, order[2], order[3]))
            rows = pl.ds(pl.multiple_of(slot * blk, blk), blk)
            total = lax.dot_general(gbuf[0, rows, :], w_ref[at, :], NT, preferred_element_type=jnp.float32)
            total += lax.dot_general(gbuf[1, rows, :], wn[at, :], NT, preferred_element_type=jnp.float32)
            cbuf[j, rows, :] = total
            for h in range(2):
                to = way(slot, h, full, pair)
                for d in range(2):
                    @pl.when(jnp.logical_and(slot == far_slot, to == d))
                    def _():
                        far_copy(j, d, h).start()

                    @pl.when(jnp.logical_and(slot == xn[d], to != d))
                    def _():
                        direct_copy(j, d, h).start()

            return 0

        lax.fori_loop(0, jnp.where(full, 4, 2), one, 0)

    def relayed(t):
        return jnp.where(t >= flush, t, jnp.maximum(t - LAG, 0))

    def step(t, _):
        gather_step(t)
        lax.fori_loop(relayed(t - 1), relayed(t), relay_step, 0)
        lax.fori_loop(jnp.maximum(t - 1 - LAST, 0), jnp.maximum(t - LAST, 0), final_step, 0)
        compute_step(t)
        return 0

    lax.fori_loop(0, n_items, step, 0)
    lax.fori_loop(n_items - 1, n_items, relay_step, 0)
    lax.fori_loop(n_items - 1 - LAST, n_items, final_step, 0)

    def drain(j, _):
        w_copy(j).wait_send()
        for h in range(2):
            far_copy(j, 0, h).wait_send()
            for d in range(2):
                direct_copy(j, d, h).wait_send()
        return 0

    lax.fori_loop(0, n_ch, drain, 0)

    def sent(sem):
        rc(g_ref, g_ref, sem, sem, partner).wait_send()

    sent(s1s.at[0])
    for d in range(2):
        for k in range(4):
            sent(zs.at[d, 0, k])
            sent(ps.at[pidx(d, 0, k)])
            if SIDE[k] == d:
                sent(zs.at[d, 1, k])
                sent(ps.at[pidx(d, 1, k)])

    @pl.when(is_src)
    def _():
        for k in range(4):
            sent(ps.at[k])
        for d in range(2):
            for k in range(4):
                if SIDE[k] != d:
                    sent(zs.at[d, 1, k])

    @pl.when(not_src)
    def _():
        sent(s1s.at[1])
        for d in range(2):
            for k in range(4):
                if SIDE[k] != d:
                    sent(ps.at[pidx(d, 1, k)])


def local(grad_out, weight):
    tb, feat = grad_out.shape
    hidden = weight.shape[0]
    n_ch = hidden // CH
    blk = 4 * tb
    dma = pltpu.SemaphoreType.DMA
    vmem = pl.BlockSpec(memory_space=pltpu.VMEM)
    hbm = pl.BlockSpec(memory_space=pltpu.HBM)
    return pl.pallas_call(
        kernel,
        out_shape=jax.ShapeDtypeStruct((blk, hidden), jnp.bfloat16),
        in_specs=[hbm, hbm],
        out_specs=vmem,
        scratch_shapes=[
            pltpu.VMEM((tb, feat), jnp.bfloat16),
            pltpu.VMEM((hidden, feat), jnp.bfloat16),
            pltpu.VMEM((2, 4 * blk, feat), jnp.bfloat16),
            pltpu.VMEM((hidden, feat), jnp.bfloat16),
            pltpu.VMEM((n_ch, 4 * blk, CH), jnp.float32),
            pltpu.VMEM((2, n_ch, 2, blk // 2, CH), jnp.float32),
            pltpu.VMEM((2, n_ch, 2, blk // 2, CH), jnp.float32),
            pltpu.VMEM((2, n_ch, blk, CH), jnp.float32),
            dma((2,)),
            dma((2,)), dma((3,)),
            dma((2, 2, 4)), dma((2, 2, 4)),
            dma((20,)), dma((20,)),
            dma((n_ch,)), dma((n_ch,)),
            dma((n_ch, 2)), dma((2, n_ch, 2)),
            dma((2, n_ch, 2)), dma((2, n_ch, 2)),
        ],
        compiler_params=pltpu.CompilerParams(
            collective_id=0, has_side_effects=True, vmem_limit_bytes=63 * 1024 * 1024
        ),
    )(grad_out, weight)


def solution(mesh):
    spec = P("col", "row")
    return jax.shard_map(local, mesh=mesh, in_specs=(spec, spec), out_specs=P("row", "col"), check_vma=False)
```

```python
import jax
import jax.numpy as jnp
from jax import lax
from jax.experimental import pallas as pl
from jax.experimental.pallas import tpu as pltpu
from jax.sharding import PartitionSpec as P

MESH = pl.DeviceIdType.MESH
CH = 128
PARTS = 2
ORDER = ((0, 0), (0, 1), (1, 0), (1, 1), (3, 0), (2, 0), (3, 1), (2, 1))
SIDE = (0, 1, 1, 0)
HALVES = 4
NT = (((1,), (1,)), ((), ()))


def kernel(
    g_hbm, w_hbm, o_ref, g_ref, w_ref, gbuf, wn, cbuf, relay, farin, nearin,
    ls, s1s, s1r, zs, zr, ps, pr, ws, wr, fs, fr, ds, dr, rs, rr,
):
    n_ch = w_ref.shape[0] // CH
    tb, feat = g_ref.shape
    blk = 4 * tb
    half = blk // 2
    row = lax.axis_index("row")
    col = lax.axis_index("col")
    x = lax.div(row, 2)
    lo = lax.rem(row, 2)
    z = lax.div(col, 4)
    hi = lax.rem(lax.div(col, 2), 2)
    c = lax.rem(col, 2)
    is_src = lax.rem(z, 2) == lo
    not_src = jnp.logical_not(is_src)

    def dev(x=x, lo=lo, z=z, hi=hi, c=c):
        return (x * 2 + lo, z * 4 + hi * 2 + c)

    zn = (lax.rem(z + 1, 8), lax.rem(z + 7, 8))
    xn = (lax.rem(x + 1, 4), lax.rem(x + 3, 4))
    partner = dev(c=1 - c)
    z_dev = (dev(z=zn[0]), dev(z=zn[1]))
    x_dev = (dev(x=xn[0]), dev(x=xn[1]))
    w_dev = dev(lo=1 - lo)
    h_dev = dev(hi=1 - hi)
    wh_dev = dev(lo=1 - lo, hi=1 - hi)

    barrier = pltpu.get_barrier_semaphore()
    peers = (partner, *z_dev, *x_dev, w_dev, h_dev, wh_dev)
    for peer in peers:
        pl.semaphore_signal(barrier, inc=1, device_id=peer, device_id_type=MESH)
    g_in = pltpu.make_async_copy(g_hbm, g_ref, ls.at[0])
    w_in = pltpu.make_async_copy(w_hbm, w_ref, ls.at[1])
    g_in.start()
    w_in.start()
    g_in.wait()
    w_in.wait()
    pl.semaphore_wait(barrier, len(peers))

    def rc(src, dst, ss, sr, to):
        return pltpu.make_async_remote_copy(
            src_ref=src, dst_ref=dst, send_sem=ss, recv_sem=sr, device_id=to, device_id_type=MESH
        )

    piece = tb // PARTS

    def place(slot, l, h, core, p):
        at = pl.multiple_of(slot * blk + (h * 2 + core) * tb + p * piece, piece)
        return gbuf.at[l, pl.ds(at, piece), :]

    def side(k):
        return lax.rem(lax.div(k + 1, 2), 2)

    def block(slot, k, core, p):
        return place(slot, side(k), lax.rem(hi + lax.div(k, 2), 2), core, p)

    def slot_of(shift):
        return lax.div(lax.rem(z + shift, 8), 2)

    s0 = lax.div(z, 2)

    def own_part(p):
        return g_ref.at[pl.ds(p * piece, piece), :]

    @pl.when(is_src)
    def _():
        for p in range(PARTS):
            own = place(s0, 0, hi, c, p)
            for d in range(2):
                rc(own_part(p), own, zs.at[d, 0, 0, p], zr.at[d, 0, 0, p], z_dev[d]).start()
            rc(own_part(p), own, s1s.at[0, p], s1r.at[2, p], h_dev).start()
            rc(own_part(p), own, ps.at[0, 0, p], pr.at[0, 0, p], partner).start()

    @pl.when(not_src)
    def _():
        for p in range(PARTS):
            there = place(s0, 1, hi, c, p)
            rc(own_part(p), there, s1s.at[0, p], s1r.at[0, p], w_dev).start()
            rc(own_part(p), there, s1s.at[1, p], s1r.at[1, p], wh_dev).start()

    def w_copy(j):
        at = pl.ds(pl.multiple_of(j * CH, CH), CH)
        return rc(w_ref.at[at, :], wn.at[at, :], ws.at[j], wr.at[j], w_dev)

    for j in range(n_ch):
        w_copy(j).start()

    def relay_to(slot, k, p, d, out_r, send_r):
        b = block(slot, k, c, p)
        rc(b, b, zs.at[d, send_r, k, p], zr.at[d, out_r, k, p], z_dev[d]).start()

    def share(slot, k, p, i):
        b = block(slot, k, c, p)
        rc(b, b, ps.at[i, k, p], pr.at[i, k, p], partner).start()

    def arrived(slot, k, p, d, r):
        b = block(slot, k, c, p)
        rc(b, b, zs.at[d, r, k, p], zr.at[d, r, k, p], z_dev[d]).wait_recv()

    def shared(slot, k, p, i):
        b = block(slot, k, 1 - c, p)
        rc(b, b, ps.at[i, k, p], pr.at[i, k, p], partner).wait_recv()

    def first_of(k, p):
        b = block(s0, k, c, p)
        rc(b, b, s1s.at[0, p], s1r.at[k - 1, p], h_dev).wait_recv()

    src_near = (slot_of(6), slot_of(2))
    opp = slot_of(4)
    mid_near = (slot_of(7), slot_of(1))
    mid_far = (slot_of(5), slot_of(3))
    early = (jnp.where(is_src, s0, mid_near[0]), jnp.where(is_src, src_near[1], mid_near[1]))
    late = (jnp.where(is_src, src_near[0], mid_far[0]), jnp.where(is_src, opp, mid_far[1]))

    def src_near_one(k, p):
        for d in range(2):
            arrived(src_near[d], k, p, d, 0)
            relay_to(src_near[d], k, p, d, 1, 1)
            share(src_near[d], k, p, 1 + d)

    def mid_near_one(k, p):
        for d in range(2):
            arrived(mid_near[d], k, p, d, 0)
            relay_to(mid_near[d], k, p, d, 0, 0)
            share(mid_near[d], k, p, 1 + d)

    def own_one(k, p):
        first_of(k, p)
        for d in range(2):
            relay_to(s0, k, p, d, 0, 0)
        share(s0, k, p, 0)

    def mid_far_one(k, p):
        for d in range(2):
            arrived(mid_far[d], k, p, d, 1)

            @pl.when(side(k) == d)
            def _():
                relay_to(mid_far[d], k, p, d, 1, 1)

            share(mid_far[d], k, p, 3 + d)

    def opp_one(ka, kb, p):
        for d, k in ((0, ka), (1, kb)):
            arrived(opp, k, p, d, 1)
            share(opp, k, p, 3)

    @pl.when(is_src)
    def _():
        gbuf[0, pl.ds(pl.multiple_of(s0 * blk + (hi * 2 + c) * tb, tb), tb), :] = g_ref[...]
        for k, p in ORDER[2:]:
            own_one(k, p)
        for k, p in ORDER:
            src_near_one(k, p)
        for p in range(PARTS):
            opp_one(0, 1, p)

    @pl.when(not_src)
    def _():
        for k, p in ORDER:
            mid_near_one(k, p)
        for k, p in ORDER[:4]:
            mid_far_one(k, p)

    def gather_step(t):
        @pl.when(jnp.logical_and(is_src, t == 3))
        def _():
            for p in range(PARTS):
                opp_one(3, 2, p)

        for p, when in ((0, 0), (1, 1)):
            @pl.when(jnp.logical_and(not_src, t == when))
            def _():
                for i in range(2):
                    mid_far_one(3 - i, p)

    def planes_ready(t):
        for when, ks in ((0, (0, 1)), (HALVES, (3, 2))):
            @pl.when(jnp.logical_and(is_src, t == when))
            def _():
                for k in ks:
                    for p in range(PARTS):
                        shared(s0, k, p, 0)
                        for d in range(2):
                            shared(src_near[d], k, p, 1 + d)
                        shared(opp, k, p, 3)

            @pl.when(jnp.logical_and(not_src, t == when))
            def _():
                for k in ks:
                    for p in range(PARTS):
                        for d in range(2):
                            shared(mid_near[d], k, p, 1 + d)
                            shared(mid_far[d], k, p, 3 + d)

    n_items = HALVES + n_ch
    far_slot = lax.rem(x + 2, 4)
    order = (far_slot, xn[0], xn[1], x)

    def group_of(t):
        full = t >= 2 * HALVES
        j = jnp.where(t < HALVES, t, t - HALVES)
        only = jnp.where(t < HALVES, hi, 1 - hi)
        return full, j, only

    def has(h, full, only):
        return jnp.logical_or(full, only == h)

    def rows_of(slot, h, q):
        return pl.ds(pl.multiple_of(slot * blk + (h * 2 + q) * tb, tb), tb)

    def far_copy(j, d, h):
        return rc(cbuf.at[j, rows_of(far_slot, h, d), :], farin.at[d, j, h], fs.at[d, j, h], fr.at[d, j, h], x_dev[d])

    def near_dst(j, d, h, q):
        return nearin.at[d, j, pl.ds((h * 2 + q) * tb, tb), :]

    def direct_copy(j, d, h):
        src = cbuf.at[j, rows_of(xn[d], h, 1 - d), :]
        return rc(src, near_dst(j, d, h, 1 - d), ds.at[d, j, h], dr.at[d, j, h], x_dev[d])

    def relay_copy(j, d, h):
        return rc(relay.at[d, j, h], near_dst(j, d, h, d), rs.at[d, j, h], rr.at[d, j, h], x_dev[d])

    def relay_step(t, _):
        full, j, only = group_of(t)
        for h in range(2):
            @pl.when(has(h, full, only))
            def _():
                for d in range(2):
                    far_copy(j, d, h).wait_recv()
                    relay[d, j, h] = cbuf[j, rows_of(xn[d], h, d), :] + farin[d, j, h]
                    relay_copy(j, d, h).start()

        return 0

    def final_step(t, _):
        full, j, only = group_of(t)
        for h in range(2):
            @pl.when(has(h, full, only))
            def _():
                for d in range(2):
                    direct_copy(j, d, h).wait_recv()
                    relay_copy(j, d, h).wait_recv()
                rows = pl.ds(h * half, half)
                mine = pl.ds(pl.multiple_of(x * blk + h * half, half), half)
                total = cbuf[j, mine, :] + nearin[0, j, rows, :] + nearin[1, j, rows, :]
                o_ref[rows, pl.ds(pl.multiple_of(j * CH, CH), CH)] = total.astype(o_ref.dtype)

        return 0

    def compute_step(t):
        full, j, only = group_of(t)

        @pl.when(jnp.logical_or(full, t < HALVES))
        def _():
            w_copy(j).wait_recv()

        at = pl.ds(pl.multiple_of(j * CH, CH), CH)

        def product(rows):
            total = lax.dot_general(gbuf[0, rows, :], w_ref[at, :], NT, preferred_element_type=jnp.float32)
            total += lax.dot_general(gbuf[1, rows, :], wn[at, :], NT, preferred_element_type=jnp.float32)
            cbuf[j, rows, :] = total

        def one(i, _):
            slot = jnp.where(i < 2, jnp.where(i == 0, order[0], order[1]), jnp.where(i == 2, order[2], order[3]))

            @pl.when(full)
            def _():
                product(pl.ds(pl.multiple_of(slot * blk, blk), blk))

            @pl.when(jnp.logical_not(full))
            def _():
                product(pl.ds(pl.multiple_of(slot * blk + only * half, half), half))

            for h in range(2):
                for d in range(2):
                    @pl.when(jnp.logical_and(has(h, full, only), i == 0))
                    def _():
                        far_copy(j, d, h).start()

                    @pl.when(jnp.logical_and(has(h, full, only), i == 1 + d))
                    def _():
                        direct_copy(j, d, h).start()

            return 0

        lax.fori_loop(0, 4, one, 0)

    def gather_sent():
        def sent(sem):
            rc(own_part(0), own_part(0), sem, sem, partner).wait_send()

        for p in range(PARTS):
            sent(s1s.at[0, p])
            for k in range(4):
                for d in range(2):
                    sent(zs.at[d, 0, k, p])
                    sent(ps.at[1 + d, k, p])
                    if SIDE[k] == d:
                        sent(zs.at[d, 1, k, p])
                sent(ps.at[3, k, p])

        @pl.when(is_src)
        def _():
            for p in range(PARTS):
                for k in range(4):
                    sent(ps.at[0, k, p])
                    sent(zs.at[1 - SIDE[k], 1, k, p])

        @pl.when(not_src)
        def _():
            for p in range(PARTS):
                sent(s1s.at[1, p])
                for k in range(4):
                    sent(ps.at[4, k, p])

    def relayed(t):
        whole = jnp.where(t >= n_items - 2, n_items - 2, jnp.maximum(t - 1, 0))
        return jnp.where(t == HALVES, t, whole)

    def finished(t):
        return jnp.where(t >= n_items - 1, n_items - 4, jnp.where(t == n_items - 2, n_items - 5, 0))

    def step(t, _):
        lax.fori_loop(relayed(t - 1), relayed(t), relay_step, 0)
        lax.fori_loop(finished(t - 1), finished(t), final_step, 0)

        @pl.when(t == n_items - 1)
        def _():
            gather_sent()

        planes_ready(t)
        compute_step(t)
        gather_step(t)
        return 0

    lax.fori_loop(0, n_items, step, 0)
    lax.fori_loop(n_items - 2, n_items - 1, relay_step, 0)
    lax.fori_loop(n_items - 4, n_items - 3, final_step, 0)
    lax.fori_loop(n_items - 1, n_items, relay_step, 0)
    lax.fori_loop(n_items - 3, n_items, final_step, 0)

    def drain(j, _):
        w_copy(j).wait_send()
        for h in range(2):
            for d in range(2):
                far_copy(j, d, h).wait_send()
                direct_copy(j, d, h).wait_send()
                relay_copy(j, d, h).wait_send()
        return 0

    lax.fori_loop(0, n_ch, drain, 0)


def local(grad_out, weight):
    tb, feat = grad_out.shape
    hidden = weight.shape[0]
    n_ch = hidden // CH
    blk = 4 * tb
    dma = pltpu.SemaphoreType.DMA
    vmem = pl.BlockSpec(memory_space=pltpu.VMEM)
    hbm = pl.BlockSpec(memory_space=pltpu.HBM)
    return pl.pallas_call(
        kernel,
        out_shape=jax.ShapeDtypeStruct((blk, hidden), jnp.bfloat16),
        in_specs=[hbm, hbm],
        out_specs=vmem,
        scratch_shapes=[
            pltpu.VMEM((tb, feat), jnp.bfloat16),
            pltpu.VMEM((hidden, feat), jnp.bfloat16),
            pltpu.VMEM((2, 4 * blk, feat), jnp.bfloat16),
            pltpu.VMEM((hidden, feat), jnp.bfloat16),
            pltpu.VMEM((n_ch, 4 * blk, CH), jnp.float32),
            pltpu.VMEM((2, n_ch, 2, tb, CH), jnp.float32),
            pltpu.VMEM((2, n_ch, 2, tb, CH), jnp.float32),
            pltpu.VMEM((2, n_ch, blk, CH), jnp.float32),
            dma((2,)),
            dma((2, PARTS)), dma((3, PARTS)),
            dma((2, 2, 4, PARTS)), dma((2, 2, 4, PARTS)),
            dma((5, 4, PARTS)), dma((5, 4, PARTS)),
            dma((n_ch,)), dma((n_ch,)),
            dma((2, n_ch, 2)), dma((2, n_ch, 2)),
            dma((2, n_ch, 2)), dma((2, n_ch, 2)),
            dma((2, n_ch, 2)), dma((2, n_ch, 2)),
        ],
        compiler_params=pltpu.CompilerParams(
            collective_id=0, has_side_effects=True, vmem_limit_bytes=63 * 1024 * 1024
        ),
    )(grad_out, weight)


def solution(mesh):
    spec = P("col", "row")
    return jax.shard_map(local, mesh=mesh, in_specs=(spec, spec), out_specs=P("row", "col"), check_vma=False)
```

```python
import jax
import jax.numpy as jnp
from jax import lax
from jax.experimental import pallas as pl
from jax.experimental.pallas import tpu as pltpu
from jax.sharding import PartitionSpec as P

MESH = pl.DeviceIdType.MESH
CH = 128
PARTS = 2
FIRST = tuple((k, p) for k in (0, 1) for p in range(PARTS))
ORDER = FIRST + tuple((k, p) for p in range(PARTS) for k in (3, 2))
SIDE = (0, 1, 1, 0)
HALVES = 4
PAIRS = (0, 4, 6, 8)
NT = (((1,), (1,)), ((), ()))


def kernel(
    g_hbm, w_hbm, o_ref, g_ref, w_ref, gbuf, wn, cbuf, relay, farin, nearin,
    ls, s1s, s1r, zs, zr, ps, pr, ws, wr, fs, fr, ds, dr, rs, rr,
):
    n_ch = w_ref.shape[0] // CH
    tb, feat = g_ref.shape
    blk = 4 * tb
    half = blk // 2
    row = lax.axis_index("row")
    col = lax.axis_index("col")
    x = lax.div(row, 2)
    lo = lax.rem(row, 2)
    z = lax.div(col, 4)
    hi = lax.rem(lax.div(col, 2), 2)
    c = lax.rem(col, 2)
    is_src = lax.rem(z, 2) == lo
    not_src = jnp.logical_not(is_src)

    def dev(x=x, lo=lo, z=z, hi=hi, c=c):
        return (x * 2 + lo, z * 4 + hi * 2 + c)

    zn = (lax.rem(z + 1, 8), lax.rem(z + 7, 8))
    xn = (lax.rem(x + 1, 4), lax.rem(x + 3, 4))
    partner = dev(c=1 - c)
    z_dev = (dev(z=zn[0]), dev(z=zn[1]))
    x_dev = (dev(x=xn[0]), dev(x=xn[1]))
    w_dev = dev(lo=1 - lo)
    h_dev = dev(hi=1 - hi)
    wh_dev = dev(lo=1 - lo, hi=1 - hi)

    barrier = pltpu.get_barrier_semaphore()
    peers = (partner, *z_dev, *x_dev, w_dev, h_dev, wh_dev)
    for peer in peers:
        pl.semaphore_signal(barrier, inc=1, device_id=peer, device_id_type=MESH)
    g_in = pltpu.make_async_copy(g_hbm, g_ref, ls.at[0])
    w_in = pltpu.make_async_copy(w_hbm, w_ref, ls.at[1])
    g_in.start()
    w_in.start()
    g_in.wait()
    w_in.wait()
    pl.semaphore_wait(barrier, len(peers))

    def rc(src, dst, ss, sr, to):
        return pltpu.make_async_remote_copy(
            src_ref=src, dst_ref=dst, send_sem=ss, recv_sem=sr, device_id=to, device_id_type=MESH
        )

    piece = tb // PARTS

    def place(slot, l, h, core, p):
        at = pl.multiple_of(slot * blk + (h * 2 + core) * tb + p * piece, piece)
        return gbuf.at[l, pl.ds(at, piece), :]

    def side(k):
        return lax.rem(lax.div(k + 1, 2), 2)

    def block(slot, k, core, p):
        return place(slot, side(k), lax.rem(hi + lax.div(k, 2), 2), core, p)

    def slot_of(shift):
        return lax.div(lax.rem(z + shift, 8), 2)

    s0 = lax.div(z, 2)

    def own_part(p):
        return g_ref.at[pl.ds(p * piece, piece), :]

    @pl.when(is_src)
    def _():
        for p in range(PARTS):
            own = place(s0, 0, hi, c, p)
            for d in range(2):
                rc(own_part(p), own, zs.at[d, 0, 0, p], zr.at[d, 0, 0, p], z_dev[d]).start()
            rc(own_part(p), own, s1s.at[0, p], s1r.at[2, p], h_dev).start()
            rc(own_part(p), own, ps.at[0, 0, p], pr.at[0, 0, p], partner).start()

    @pl.when(not_src)
    def _():
        for p in range(PARTS):
            there = place(s0, 1, hi, c, p)
            rc(own_part(p), there, s1s.at[0, p], s1r.at[0, p], w_dev).start()
            rc(own_part(p), there, s1s.at[1, p], s1r.at[1, p], wh_dev).start()

    def w_copy(j):
        at = pl.ds(pl.multiple_of(j * CH, CH), CH)
        return rc(w_ref.at[at, :], wn.at[at, :], ws.at[j], wr.at[j], w_dev)

    for j in range(n_ch):
        w_copy(j).start()

    def relay_to(slot, k, p, d, out_r, send_r):
        b = block(slot, k, c, p)
        rc(b, b, zs.at[d, send_r, k, p], zr.at[d, out_r, k, p], z_dev[d]).start()

    def share(slot, k, p, i):
        b = block(slot, k, c, p)
        rc(b, b, ps.at[i, k, p], pr.at[i, k, p], partner).start()

    def arrived(slot, k, p, d, r):
        b = block(slot, k, c, p)
        rc(b, b, zs.at[d, r, k, p], zr.at[d, r, k, p], z_dev[d]).wait_recv()

    def shared(slot, k, p, i):
        b = block(slot, k, 1 - c, p)
        rc(b, b, ps.at[i, k, p], pr.at[i, k, p], partner).wait_recv()

    def first_of(k, p):
        b = block(s0, k, c, p)
        rc(b, b, s1s.at[0, p], s1r.at[k - 1, p], h_dev).wait_recv()

    src_near = (slot_of(6), slot_of(2))
    opp = slot_of(4)
    mid_near = (slot_of(7), slot_of(1))
    mid_far = (slot_of(5), slot_of(3))
    early = (jnp.where(is_src, s0, mid_near[0]), jnp.where(is_src, src_near[1], mid_near[1]))
    late = (jnp.where(is_src, src_near[0], mid_far[0]), jnp.where(is_src, opp, mid_far[1]))

    def src_near_one(k, p):
        for d in range(2):
            arrived(src_near[d], k, p, d, 0)
            relay_to(src_near[d], k, p, d, 1, 1)
            share(src_near[d], k, p, 1 + d)

    def mid_near_one(k, p):
        for d in range(2):
            arrived(mid_near[d], k, p, d, 0)
            relay_to(mid_near[d], k, p, d, 0, 0)
            share(mid_near[d], k, p, 1 + d)

    def own_one(k, p):
        first_of(k, p)
        for d in range(2):
            relay_to(s0, k, p, d, 0, 0)
        share(s0, k, p, 0)

    def mid_far_one(k, p):
        for d in range(2):
            arrived(mid_far[d], k, p, d, 1)

            @pl.when(side(k) == d)
            def _():
                relay_to(mid_far[d], k, p, d, 1, 1)

            share(mid_far[d], k, p, 3 + d)

    def opp_one(ka, kb, p):
        for d, k in ((0, ka), (1, kb)):
            arrived(opp, k, p, d, 1)
            share(opp, k, p, 3)

    @pl.when(is_src)
    def _():
        gbuf[0, pl.ds(pl.multiple_of(s0 * blk + (hi * 2 + c) * tb, tb), tb), :] = g_ref[...]
        for k, p in ORDER[PARTS:]:
            own_one(k, p)
        for k, p in ORDER:
            src_near_one(k, p)
        for p in range(PARTS):
            opp_one(0, 1, p)

    @pl.when(not_src)
    def _():
        for k, p in ORDER:
            mid_near_one(k, p)
        for k, p in FIRST:
            mid_far_one(k, p)

    def gather_step(t):
        @pl.when(jnp.logical_and(is_src, t == 3))
        def _():
            for p in range(PARTS):
                opp_one(3, 2, p)

        for when in range(2):
            @pl.when(jnp.logical_and(not_src, t == when))
            def _():
                for p in range(when * PARTS // 2, (when + 1) * PARTS // 2):
                    for k in (3, 2):
                        mid_far_one(k, p)

    def planes_ready(t):
        for when, ks in ((0, (0, 1)), (HALVES, (3, 2))):
            @pl.when(jnp.logical_and(is_src, t == when))
            def _():
                for k in ks:
                    for p in range(PARTS):
                        shared(s0, k, p, 0)
                        for d in range(2):
                            shared(src_near[d], k, p, 1 + d)
                        shared(opp, k, p, 3)

            @pl.when(jnp.logical_and(not_src, t == when))
            def _():
                for k in ks:
                    for p in range(PARTS):
                        for d in range(2):
                            shared(mid_near[d], k, p, 1 + d)
                            shared(mid_far[d], k, p, 3 + d)

    n_items = HALVES + n_ch
    far_slot = lax.rem(x + 2, 4)
    order = (far_slot, xn[0], xn[1], x)

    def group_of(t):
        full = t >= 2 * HALVES
        j = jnp.where(t < HALVES, t, t - HALVES)
        only = jnp.where(t < HALVES, hi, 1 - hi)
        return full, j, only

    def has(h, full, only):
        return jnp.logical_or(full, only == h)

    def rows_of(slot, h, q):
        return pl.ds(pl.multiple_of(slot * blk + (h * 2 + q) * tb, tb), tb)

    def far_copy(j, d, h):
        return rc(cbuf.at[j, rows_of(far_slot, h, d), :], farin.at[d, j, h], fs.at[d, j, h], fr.at[d, j, h], x_dev[d])

    def near_dst(j, d, h, q):
        return nearin.at[d, j, pl.ds((h * 2 + q) * tb, tb), :]

    def direct_copy(j, d, h):
        src = cbuf.at[j, rows_of(xn[d], h, 1 - d), :]
        return rc(src, near_dst(j, d, h, 1 - d), ds.at[d, j, h], dr.at[d, j, h], x_dev[d])

    def relay_copy(j, d, h):
        return rc(relay.at[d, j, h], near_dst(j, d, h, d), rs.at[d, j, h], rr.at[d, j, h], x_dev[d])

    def relay_step(t, _):
        full, j, only = group_of(t)
        for h in range(2):
            @pl.when(has(h, full, only))
            def _():
                for d in range(2):
                    far_copy(j, d, h).wait_recv()
                    relay[d, j, h] = cbuf[j, rows_of(xn[d], h, d), :] + farin[d, j, h]
                    relay_copy(j, d, h).start()

        return 0

    def final_step(t, _):
        full, j, only = group_of(t)
        for h in range(2):
            @pl.when(has(h, full, only))
            def _():
                for d in range(2):
                    direct_copy(j, d, h).wait_recv()
                    relay_copy(j, d, h).wait_recv()
                rows = pl.ds(h * half, half)
                mine = pl.ds(pl.multiple_of(x * blk + h * half, half), half)
                total = cbuf[j, mine, :] + nearin[0, j, rows, :] + nearin[1, j, rows, :]
                o_ref[rows, pl.ds(pl.multiple_of(j * CH, CH), CH)] = total.astype(o_ref.dtype)

        return 0

    def compute_step(t):
        full, j, only = group_of(t)
        paired = sum((t == i).astype(jnp.int32) for i in PAIRS) > 0

        after = sum((t == i + 1).astype(jnp.int32) for i in PAIRS)

        @pl.when(jnp.logical_and(after == 0, jnp.logical_or(full, t < HALVES)))
        def _():
            w_copy(j).wait_recv()

            @pl.when(paired)
            def _():
                w_copy(j + 1).wait_recv()

        def product(rows, wide):
            at = pl.ds(pl.multiple_of(j * CH, CH), wide * CH)
            total = lax.dot_general(gbuf[0, rows, :], w_ref[at, :], NT, preferred_element_type=jnp.float32)
            total += lax.dot_general(gbuf[1, rows, :], wn[at, :], NT, preferred_element_type=jnp.float32)
            for i in range(wide):
                cbuf[j + i, rows, :] = total[:, i * CH : (i + 1) * CH]

        def one(i, _):
            slot = jnp.where(i < 2, jnp.where(i == 0, order[0], order[1]), jnp.where(i == 2, order[2], order[3]))
            for wide in (1, 2):
                this = paired if wide == 2 else jnp.logical_not(paired)

                @pl.when(jnp.logical_and(this, full))
                def _():
                    product(pl.ds(pl.multiple_of(slot * blk, blk), blk), wide)

                @pl.when(jnp.logical_and(this, jnp.logical_not(full)))
                def _():
                    product(pl.ds(pl.multiple_of(slot * blk + only * half, half), half), wide)

            def send(n, _):
                for h in range(2):
                    for d in range(2):
                        @pl.when(jnp.logical_and(has(h, full, only), i == 0))
                        def _():
                            far_copy(j + n, d, h).start()

                        @pl.when(jnp.logical_and(has(h, full, only), i == 1 + d))
                        def _():
                            direct_copy(j + n, d, h).start()

                return 0

            lax.fori_loop(0, jnp.where(paired, 2, 1), send, 0)
            return 0

        @pl.when(after == 0)
        def _():
            lax.fori_loop(0, 4, one, 0)

    def gather_sent():
        def sent(sem):
            rc(own_part(0), own_part(0), sem, sem, partner).wait_send()

        for p in range(PARTS):
            sent(s1s.at[0, p])
            for k in range(4):
                for d in range(2):
                    sent(zs.at[d, 0, k, p])
                    sent(ps.at[1 + d, k, p])
                    if SIDE[k] == d:
                        sent(zs.at[d, 1, k, p])
                sent(ps.at[3, k, p])

        @pl.when(is_src)
        def _():
            for p in range(PARTS):
                for k in range(4):
                    sent(ps.at[0, k, p])
                    sent(zs.at[1 - SIDE[k], 1, k, p])

        @pl.when(not_src)
        def _():
            for p in range(PARTS):
                sent(s1s.at[1, p])
                for k in range(4):
                    sent(ps.at[4, k, p])

    def relayed(t):
        return jnp.clip(t - 2, 0, n_items - 3)

    def finished(t):
        return jnp.where(t >= n_items - 2, n_items - 6, 0)

    def drain(j, _):
        w_copy(j).wait_send()
        for h in range(2):
            for d in range(2):
                far_copy(j, d, h).wait_send()
                direct_copy(j, d, h).wait_send()
                relay_copy(j, d, h).wait_send()
        return 0

    def step(t, _):
        lax.fori_loop(relayed(t - 1), relayed(t), relay_step, 0)
        lax.fori_loop(finished(t - 1), finished(t), final_step, 0)

        planes_ready(t)
        compute_step(t)
        gather_step(t)
        return 0

    lax.fori_loop(0, n_items, step, 0)
    lax.fori_loop(n_items - 3, n_items - 2, relay_step, 0)
    lax.fori_loop(n_items - 6, n_items - 4, final_step, 0)
    lax.fori_loop(n_items - 2, n_items, relay_step, 0)
    gather_sent()
    lax.fori_loop(0, n_ch - 3, drain, 0)
    lax.fori_loop(n_items - 4, n_items, final_step, 0)
    lax.fori_loop(n_ch - 3, n_ch, drain, 0)


def local(grad_out, weight):
    tb, feat = grad_out.shape
    hidden = weight.shape[0]
    n_ch = hidden // CH
    blk = 4 * tb
    dma = pltpu.SemaphoreType.DMA
    vmem = pl.BlockSpec(memory_space=pltpu.VMEM)
    hbm = pl.BlockSpec(memory_space=pltpu.HBM)
    return pl.pallas_call(
        kernel,
        out_shape=jax.ShapeDtypeStruct((blk, hidden), jnp.bfloat16),
        in_specs=[hbm, hbm],
        out_specs=vmem,
        scratch_shapes=[
            pltpu.VMEM((tb, feat), jnp.bfloat16),
            pltpu.VMEM((hidden, feat), jnp.bfloat16),
            pltpu.VMEM((2, 4 * blk, feat), jnp.bfloat16),
            pltpu.VMEM((hidden, feat), jnp.bfloat16),
            pltpu.VMEM((n_ch, 4 * blk, CH), jnp.float32),
            pltpu.VMEM((2, n_ch, 2, tb, CH), jnp.float32),
            pltpu.VMEM((2, n_ch, 2, tb, CH), jnp.float32),
            pltpu.VMEM((2, n_ch, blk, CH), jnp.float32),
            dma((2,)),
            dma((2, PARTS)), dma((3, PARTS)),
            dma((2, 2, 4, PARTS)), dma((2, 2, 4, PARTS)),
            dma((5, 4, PARTS)), dma((5, 4, PARTS)),
            dma((n_ch,)), dma((n_ch,)),
            dma((2, n_ch, 2)), dma((2, n_ch, 2)),
            dma((2, n_ch, 2)), dma((2, n_ch, 2)),
            dma((2, n_ch, 2)), dma((2, n_ch, 2)),
        ],
        compiler_params=pltpu.CompilerParams(
            collective_id=0, has_side_effects=True, vmem_limit_bytes=63 * 1024 * 1024
        ),
    )(grad_out, weight)


def solution(mesh):
    spec = P("col", "row")
    return jax.shard_map(local, mesh=mesh, in_specs=(spec, spec), out_specs=P("row", "col"), check_vma=False)
```

```python
import jax
import jax.numpy as jnp
from jax import lax
from jax.experimental import pallas as pl
from jax.experimental.pallas import tpu as pltpu
from jax.sharding import PartitionSpec as P

MESH = pl.DeviceIdType.MESH
CH = 128
PARTS = 2
FIRST = tuple((k, p) for k in (0, 1) for p in range(PARTS))
ORDER = FIRST + tuple((k, p) for p in range(PARTS) for k in (3, 2))
SIDE = (0, 1, 1, 0)
HALVES = 4
PAIRS = (0, 4, 6, 8)
NT = (((1,), (1,)), ((), ()))


def kernel(
    g_hbm, w_hbm, o_ref, g_ref, w_ref, gbuf, wn, cbuf, relay, farin, nearin,
    ls, s1s, s1r, zs, zr, ps, pr, ws, wr, fs, fr, ds, dr, rs, rr,
):
    n_ch = w_ref.shape[0] // CH
    tb, feat = g_ref.shape
    blk = 4 * tb
    half = blk // 2
    row = lax.axis_index("row")
    col = lax.axis_index("col")
    x = lax.div(row, 2)
    lo = lax.rem(row, 2)
    z = lax.div(col, 4)
    hi = lax.rem(lax.div(col, 2), 2)
    c = lax.rem(col, 2)
    is_src = lax.rem(z, 2) == lo
    not_src = jnp.logical_not(is_src)

    def dev(x=x, lo=lo, z=z, hi=hi, c=c):
        return (x * 2 + lo, z * 4 + hi * 2 + c)

    zn = (lax.rem(z + 1, 8), lax.rem(z + 7, 8))
    xn = (lax.rem(x + 1, 4), lax.rem(x + 3, 4))
    partner = dev(c=1 - c)
    z_dev = (dev(z=zn[0]), dev(z=zn[1]))
    x_dev = (dev(x=xn[0]), dev(x=xn[1]))
    w_dev = dev(lo=1 - lo)
    h_dev = dev(hi=1 - hi)
    wh_dev = dev(lo=1 - lo, hi=1 - hi)

    barrier = pltpu.get_barrier_semaphore()
    peers = (partner, *z_dev, *x_dev, w_dev, h_dev, wh_dev)
    for peer in peers:
        pl.semaphore_signal(barrier, inc=1, device_id=peer, device_id_type=MESH)
    g_in = pltpu.make_async_copy(g_hbm, g_ref, ls.at[0])
    w_in = pltpu.make_async_copy(w_hbm, w_ref, ls.at[1])
    g_in.start()
    w_in.start()
    g_in.wait()
    w_in.wait()
    pl.semaphore_wait(barrier, len(peers))

    def rc(src, dst, ss, sr, to):
        return pltpu.make_async_remote_copy(
            src_ref=src, dst_ref=dst, send_sem=ss, recv_sem=sr, device_id=to, device_id_type=MESH
        )

    piece = tb // PARTS

    def place(slot, l, h, core, p):
        at = pl.multiple_of(slot * blk + (h * 2 + core) * tb + p * piece, piece)
        return gbuf.at[l, pl.ds(at, piece), :]

    def side(k):
        return lax.rem(lax.div(k + 1, 2), 2)

    def block(slot, k, core, p):
        return place(slot, side(k), lax.rem(hi + lax.div(k, 2), 2), core, p)

    def slot_of(shift):
        return lax.div(lax.rem(z + shift, 8), 2)

    s0 = lax.div(z, 2)

    def own_part(p):
        return g_ref.at[pl.ds(p * piece, piece), :]

    @pl.when(is_src)
    def _():
        for p in range(PARTS):
            own = place(s0, 0, hi, c, p)
            for d in range(2):
                rc(own_part(p), own, zs.at[d, 0, 0, p], zr.at[d, 0, 0, p], z_dev[d]).start()
            rc(own_part(p), own, s1s.at[0, p], s1r.at[2, p], h_dev).start()
            rc(own_part(p), own, ps.at[0, 0, p], pr.at[0, 0, p], partner).start()

    @pl.when(not_src)
    def _():
        for p in range(PARTS):
            there = place(s0, 1, hi, c, p)
            rc(own_part(p), there, s1s.at[0, p], s1r.at[0, p], w_dev).start()
            rc(own_part(p), there, s1s.at[1, p], s1r.at[1, p], wh_dev).start()

    def w_copy(j):
        at = pl.ds(pl.multiple_of(j * CH, CH), CH)
        return rc(w_ref.at[at, :], wn.at[at, :], ws.at[j], wr.at[j], w_dev)

    for j in range(n_ch):
        w_copy(j).start()

    def relay_to(slot, k, p, d, out_r, send_r):
        b = block(slot, k, c, p)
        rc(b, b, zs.at[d, send_r, k, p], zr.at[d, out_r, k, p], z_dev[d]).start()

    def share(slot, k, p, i):
        b = block(slot, k, c, p)
        rc(b, b, ps.at[i, k, p], pr.at[i, k, p], partner).start()

    def arrived(slot, k, p, d, r):
        b = block(slot, k, c, p)
        rc(b, b, zs.at[d, r, k, p], zr.at[d, r, k, p], z_dev[d]).wait_recv()

    def shared(slot, k, p, i):
        b = block(slot, k, 1 - c, p)
        rc(b, b, ps.at[i, k, p], pr.at[i, k, p], partner).wait_recv()

    def first_of(k, p):
        b = block(s0, k, c, p)
        rc(b, b, s1s.at[0, p], s1r.at[k - 1, p], h_dev).wait_recv()

    src_near = (slot_of(6), slot_of(2))
    opp = slot_of(4)
    mid_near = (slot_of(7), slot_of(1))
    mid_far = (slot_of(5), slot_of(3))
    early = (jnp.where(is_src, s0, mid_near[0]), jnp.where(is_src, src_near[1], mid_near[1]))
    late = (jnp.where(is_src, src_near[0], mid_far[0]), jnp.where(is_src, opp, mid_far[1]))

    def src_near_one(k, p):
        for d in range(2):
            arrived(src_near[d], k, p, d, 0)
            relay_to(src_near[d], k, p, d, 1, 1)
            share(src_near[d], k, p, 1 + d)

    def mid_near_one(k, p):
        for d in range(2):
            arrived(mid_near[d], k, p, d, 0)
            relay_to(mid_near[d], k, p, d, 0, 0)
            share(mid_near[d], k, p, 1 + d)

    def own_one(k, p):
        first_of(k, p)
        for d in range(2):
            relay_to(s0, k, p, d, 0, 0)
        share(s0, k, p, 0)

    def mid_far_one(k, p):
        for d in range(2):
            arrived(mid_far[d], k, p, d, 1)

            @pl.when(side(k) == d)
            def _():
                relay_to(mid_far[d], k, p, d, 1, 1)

            share(mid_far[d], k, p, 3 + d)

    def opp_one(ka, kb, p):
        for d, k in ((0, ka), (1, kb)):
            arrived(opp, k, p, d, 1)
            share(opp, k, p, 3)

    @pl.when(is_src)
    def _():
        gbuf[0, pl.ds(pl.multiple_of(s0 * blk + (hi * 2 + c) * tb, tb), tb), :] = g_ref[...]
        for k, p in ORDER[PARTS:]:
            own_one(k, p)
        for k, p in ORDER:
            src_near_one(k, p)
        for p in range(PARTS):
            opp_one(0, 1, p)

    @pl.when(not_src)
    def _():
        for k, p in ORDER:
            mid_near_one(k, p)
        for k, p in FIRST:
            mid_far_one(k, p)

    def gather_step(t):
        @pl.when(jnp.logical_and(is_src, t == 3))
        def _():
            for p in range(PARTS):
                opp_one(3, 2, p)

        for when in range(2):
            @pl.when(jnp.logical_and(not_src, t == when))
            def _():
                for p in range(when * PARTS // 2, (when + 1) * PARTS // 2):
                    for k in (3, 2):
                        mid_far_one(k, p)

    def planes_ready(t):
        for when, ks in ((0, (0, 1)), (HALVES, (3, 2))):
            @pl.when(jnp.logical_and(is_src, t == when))
            def _():
                for k in ks:
                    for p in range(PARTS):
                        shared(s0, k, p, 0)
                        for d in range(2):
                            shared(src_near[d], k, p, 1 + d)
                        shared(opp, k, p, 3)

            @pl.when(jnp.logical_and(not_src, t == when))
            def _():
                for k in ks:
                    for p in range(PARTS):
                        for d in range(2):
                            shared(mid_near[d], k, p, 1 + d)
                            shared(mid_far[d], k, p, 3 + d)

    n_items = HALVES + n_ch
    far_slot = lax.rem(x + 2, 4)
    order = (far_slot, xn[0], xn[1], x)

    def group_of(t):
        full = t >= 2 * HALVES
        j = jnp.where(t < HALVES, t, t - HALVES)
        only = jnp.where(t < HALVES, hi, 1 - hi)
        return full, j, only

    def has(h, full, only):
        return jnp.logical_or(full, only == h)

    def rows_of(slot, h, q):
        return pl.ds(pl.multiple_of(slot * blk + (h * 2 + q) * tb, tb), tb)

    def far_copy(j, d, h):
        return rc(cbuf.at[j, rows_of(far_slot, h, d), :], farin.at[d, j, h], fs.at[d, j, h], fr.at[d, j, h], x_dev[d])

    def near_dst(j, d, h, q):
        return nearin.at[d, j, pl.ds((h * 2 + q) * tb, tb), :]

    def direct_copy(j, d, h):
        src = cbuf.at[j, rows_of(xn[d], h, 1 - d), :]
        return rc(src, near_dst(j, d, h, 1 - d), ds.at[d, j, h], dr.at[d, j, h], x_dev[d])

    def relay_copy(j, d, h):
        return rc(relay.at[d, j, h], near_dst(j, d, h, d), rs.at[d, j, h], rr.at[d, j, h], x_dev[d])

    def relay_step(t, _):
        full, j, only = group_of(t)
        for h in range(2):
            @pl.when(has(h, full, only))
            def _():
                for d in range(2):
                    far_copy(j, d, h).wait_recv()
                    relay[d, j, h] = cbuf[j, rows_of(xn[d], h, d), :] + farin[d, j, h]
                    relay_copy(j, d, h).start()

        return 0

    def final_step(t, _):
        full, j, only = group_of(t)
        for h in range(2):
            @pl.when(has(h, full, only))
            def _():
                for d in range(2):
                    direct_copy(j, d, h).wait_recv()
                    relay_copy(j, d, h).wait_recv()
                rows = pl.ds(h * half, half)
                mine = pl.ds(pl.multiple_of(x * blk + h * half, half), half)
                total = cbuf[j, mine, :] + nearin[0, j, rows, :] + nearin[1, j, rows, :]
                o_ref[rows, pl.ds(pl.multiple_of(j * CH, CH), CH)] = total.astype(o_ref.dtype)

        return 0

    def compute_step(t):
        full, j, only = group_of(t)
        paired = sum((t == i).astype(jnp.int32) for i in PAIRS) > 0

        after = sum((t == i + 1).astype(jnp.int32) for i in PAIRS)

        @pl.when(jnp.logical_and(after == 0, jnp.logical_or(full, t < HALVES)))
        def _():
            w_copy(j).wait_recv()

            @pl.when(paired)
            def _():
                w_copy(j + 1).wait_recv()

        def product(rows, wide):
            at = pl.ds(pl.multiple_of(j * CH, CH), wide * CH)
            total = lax.dot_general(gbuf[0, rows, :], w_ref[at, :], NT, preferred_element_type=jnp.float32)
            total += lax.dot_general(gbuf[1, rows, :], wn[at, :], NT, preferred_element_type=jnp.float32)
            for i in range(wide):
                cbuf[j + i, rows, :] = total[:, i * CH : (i + 1) * CH]

        def one(i, _):
            slot = jnp.where(i < 2, jnp.where(i == 0, order[0], order[1]), jnp.where(i == 2, order[2], order[3]))
            for wide in (1, 2):
                this = paired if wide == 2 else jnp.logical_not(paired)

                @pl.when(jnp.logical_and(this, full))
                def _():
                    product(pl.ds(pl.multiple_of(slot * blk, blk), blk), wide)

                @pl.when(jnp.logical_and(this, jnp.logical_not(full)))
                def _():
                    product(pl.ds(pl.multiple_of(slot * blk + only * half, half), half), wide)

            def send(n, _):
                for h in range(2):
                    for d in range(2):
                        @pl.when(jnp.logical_and(has(h, full, only), i == 0))
                        def _():
                            far_copy(j + n, d, h).start()

                        @pl.when(jnp.logical_and(has(h, full, only), i == 1 + d))
                        def _():
                            direct_copy(j + n, d, h).start()

                return 0

            lax.fori_loop(0, jnp.where(paired, 2, 1), send, 0)
            return 0

        @pl.when(after == 0)
        def _():
            lax.fori_loop(0, 4, one, 0)

    def gather_sent():
        def sent(sem):
            rc(own_part(0), own_part(0), sem, sem, partner).wait_send()

        for p in range(PARTS):
            sent(s1s.at[0, p])
            for k in range(4):
                for d in range(2):
                    sent(zs.at[d, 0, k, p])
                    sent(ps.at[1 + d, k, p])
                    if SIDE[k] == d:
                        sent(zs.at[d, 1, k, p])
                sent(ps.at[3, k, p])

        @pl.when(is_src)
        def _():
            for p in range(PARTS):
                for k in range(4):
                    sent(ps.at[0, k, p])
                    sent(zs.at[1 - SIDE[k], 1, k, p])

        @pl.when(not_src)
        def _():
            for p in range(PARTS):
                sent(s1s.at[1, p])
                for k in range(4):
                    sent(ps.at[4, k, p])

    def relayed(t):
        return jnp.clip(t - 2, 0, n_items - 3)

    def finished(t):
        return jnp.where(t >= n_items - 2, n_items - 8, 0)

    def drain(j, _):
        w_copy(j).wait_send()
        for h in range(2):
            for d in range(2):
                far_copy(j, d, h).wait_send()
                direct_copy(j, d, h).wait_send()
                relay_copy(j, d, h).wait_send()
        return 0

    def step(t, _):
        lax.fori_loop(relayed(t - 1), relayed(t), relay_step, 0)
        lax.fori_loop(finished(t - 1), finished(t), final_step, 0)

        planes_ready(t)
        compute_step(t)
        gather_step(t)
        return 0

    lax.fori_loop(0, n_items, step, 0)
    lax.fori_loop(n_items - 3, n_items - 1, relay_step, 0)
    lax.fori_loop(n_items - 8, n_items - 6, final_step, 0)
    lax.fori_loop(n_items - 1, n_items, relay_step, 0)
    gather_sent()
    lax.fori_loop(0, n_ch - 3, drain, 0)
    lax.fori_loop(n_items - 6, n_items, final_step, 0)
    lax.fori_loop(n_ch - 3, n_ch, drain, 0)


def local(grad_out, weight):
    tb, feat = grad_out.shape
    hidden = weight.shape[0]
    n_ch = hidden // CH
    blk = 4 * tb
    dma = pltpu.SemaphoreType.DMA
    vmem = pl.BlockSpec(memory_space=pltpu.VMEM)
    hbm = pl.BlockSpec(memory_space=pltpu.HBM)
    return pl.pallas_call(
        kernel,
        out_shape=jax.ShapeDtypeStruct((blk, hidden), jnp.bfloat16),
        in_specs=[hbm, hbm],
        out_specs=vmem,
        scratch_shapes=[
            pltpu.VMEM((tb, feat), jnp.bfloat16),
            pltpu.VMEM((hidden, feat), jnp.bfloat16),
            pltpu.VMEM((2, 4 * blk, feat), jnp.bfloat16),
            pltpu.VMEM((hidden, feat), jnp.bfloat16),
            pltpu.VMEM((n_ch, 4 * blk, CH), jnp.float32),
            pltpu.VMEM((2, n_ch, 2, tb, CH), jnp.float32),
            pltpu.VMEM((2, n_ch, 2, tb, CH), jnp.float32),
            pltpu.VMEM((2, n_ch, blk, CH), jnp.float32),
            dma((2,)),
            dma((2, PARTS)), dma((3, PARTS)),
            dma((2, 2, 4, PARTS)), dma((2, 2, 4, PARTS)),
            dma((5, 4, PARTS)), dma((5, 4, PARTS)),
            dma((n_ch,)), dma((n_ch,)),
            dma((2, n_ch, 2)), dma((2, n_ch, 2)),
            dma((2, n_ch, 2)), dma((2, n_ch, 2)),
            dma((2, n_ch, 2)), dma((2, n_ch, 2)),
        ],
        compiler_params=pltpu.CompilerParams(
            collective_id=0, has_side_effects=True, vmem_limit_bytes=63 * 1024 * 1024
        ),
    )(grad_out, weight)


def solution(mesh):
    spec = P("col", "row")
    return jax.shard_map(local, mesh=mesh, in_specs=(spec, spec), out_specs=P("row", "col"), check_vma=False)
```

```python
import jax
import jax.numpy as jnp
from jax import lax
from jax.experimental import pallas as pl
from jax.experimental.pallas import tpu as pltpu
from jax.sharding import PartitionSpec as P

MESH = pl.DeviceIdType.MESH
CH = 128
PARTS = 2
FIRST = tuple((k, p) for k in (0, 1) for p in range(PARTS))
ORDER = FIRST + tuple((k, p) for p in range(PARTS) for k in (3, 2))
SIDE = (0, 1, 1, 0)
HALVES = 4
PAIRS = (0, 4, 6, 8)
NT = (((1,), (1,)), ((), ()))


def kernel(
    g_hbm, w_hbm, o_ref, g_ref, w_ref, gbuf, wn, cbuf, relay, farin, nearin,
    ls, s1s, s1r, zs, zr, ps, pr, ws, wr, fs, fr, ds, dr, rs, rr,
):
    n_ch = w_ref.shape[0] // CH
    tb, feat = g_ref.shape
    blk = 4 * tb
    half = blk // 2
    row = lax.axis_index("row")
    col = lax.axis_index("col")
    x = lax.div(row, 2)
    lo = lax.rem(row, 2)
    z = lax.div(col, 4)
    hi = lax.rem(lax.div(col, 2), 2)
    c = lax.rem(col, 2)
    is_src = lax.rem(z, 2) == lo
    not_src = jnp.logical_not(is_src)

    def dev(x=x, lo=lo, z=z, hi=hi, c=c):
        return (x * 2 + lo, z * 4 + hi * 2 + c)

    zn = (lax.rem(z + 1, 8), lax.rem(z + 7, 8))
    xn = (lax.rem(x + 1, 4), lax.rem(x + 3, 4))
    partner = dev(c=1 - c)
    z_dev = (dev(z=zn[0]), dev(z=zn[1]))
    x_dev = (dev(x=xn[0]), dev(x=xn[1]))
    w_dev = dev(lo=1 - lo)
    h_dev = dev(hi=1 - hi)
    wh_dev = dev(lo=1 - lo, hi=1 - hi)

    g_in = pltpu.make_async_copy(g_hbm, g_ref, ls.at[0])
    g_in.start()
    barrier = pltpu.get_barrier_semaphore()
    peers = (partner, *z_dev, *x_dev, w_dev, h_dev, wh_dev)
    for peer in peers:
        pl.semaphore_signal(barrier, inc=1, device_id=peer, device_id_type=MESH)
    w_in = pltpu.make_async_copy(w_hbm, w_ref, ls.at[1])
    w_in.start()
    g_in.wait()
    pl.semaphore_wait(barrier, len(peers))

    def rc(src, dst, ss, sr, to):
        return pltpu.make_async_remote_copy(
            src_ref=src, dst_ref=dst, send_sem=ss, recv_sem=sr, device_id=to, device_id_type=MESH
        )

    piece = tb // PARTS

    def place(slot, l, h, core, p):
        at = pl.multiple_of(slot * blk + (h * 2 + core) * tb + p * piece, piece)
        return gbuf.at[l, pl.ds(at, piece), :]

    def side(k):
        return lax.rem(lax.div(k + 1, 2), 2)

    def block(slot, k, core, p):
        return place(slot, side(k), lax.rem(hi + lax.div(k, 2), 2), core, p)

    def slot_of(shift):
        return lax.div(lax.rem(z + shift, 8), 2)

    s0 = lax.div(z, 2)

    def own_part(p):
        return g_ref.at[pl.ds(p * piece, piece), :]

    @pl.when(is_src)
    def _():
        for p in range(PARTS):
            own = place(s0, 0, hi, c, p)
            for d in range(2):
                rc(own_part(p), own, zs.at[d, 0, 0, p], zr.at[d, 0, 0, p], z_dev[d]).start()
            rc(own_part(p), own, s1s.at[0, p], s1r.at[2, p], h_dev).start()
            rc(own_part(p), own, ps.at[0, 0, p], pr.at[0, 0, p], partner).start()

    @pl.when(not_src)
    def _():
        for p in range(PARTS):
            there = place(s0, 1, hi, c, p)
            rc(own_part(p), there, s1s.at[0, p], s1r.at[0, p], w_dev).start()
            rc(own_part(p), there, s1s.at[1, p], s1r.at[1, p], wh_dev).start()

    def w_copy(j):
        at = pl.ds(pl.multiple_of(j * CH, CH), CH)
        return rc(w_ref.at[at, :], wn.at[at, :], ws.at[j], wr.at[j], w_dev)

    w_in.wait()
    for j in range(n_ch):
        w_copy(j).start()

    def relay_to(slot, k, p, d, out_r, send_r):
        b = block(slot, k, c, p)
        rc(b, b, zs.at[d, send_r, k, p], zr.at[d, out_r, k, p], z_dev[d]).start()

    def share(slot, k, p, i):
        b = block(slot, k, c, p)
        rc(b, b, ps.at[i, k, p], pr.at[i, k, p], partner).start()

    def arrived(slot, k, p, d, r):
        b = block(slot, k, c, p)
        rc(b, b, zs.at[d, r, k, p], zr.at[d, r, k, p], z_dev[d]).wait_recv()

    def shared(slot, k, p, i):
        b = block(slot, k, 1 - c, p)
        rc(b, b, ps.at[i, k, p], pr.at[i, k, p], partner).wait_recv()

    def first_of(k, p):
        b = block(s0, k, c, p)
        rc(b, b, s1s.at[0, p], s1r.at[k - 1, p], h_dev).wait_recv()

    src_near = (slot_of(6), slot_of(2))
    opp = slot_of(4)
    mid_near = (slot_of(7), slot_of(1))
    mid_far = (slot_of(5), slot_of(3))
    early = (jnp.where(is_src, s0, mid_near[0]), jnp.where(is_src, src_near[1], mid_near[1]))
    late = (jnp.where(is_src, src_near[0], mid_far[0]), jnp.where(is_src, opp, mid_far[1]))

    def src_near_one(k, p):
        for d in range(2):
            arrived(src_near[d], k, p, d, 0)
            relay_to(src_near[d], k, p, d, 1, 1)
            share(src_near[d], k, p, 1 + d)

    def mid_near_one(k, p):
        for d in range(2):
            arrived(mid_near[d], k, p, d, 0)
            relay_to(mid_near[d], k, p, d, 0, 0)
            share(mid_near[d], k, p, 1 + d)

    def own_one(k, p):
        first_of(k, p)
        for d in range(2):
            relay_to(s0, k, p, d, 0, 0)
        share(s0, k, p, 0)

    def mid_far_one(k, p):
        for d in range(2):
            arrived(mid_far[d], k, p, d, 1)

            @pl.when(side(k) == d)
            def _():
                relay_to(mid_far[d], k, p, d, 1, 1)

            share(mid_far[d], k, p, 3 + d)

    def opp_one(ka, kb, p):
        for d, k in ((0, ka), (1, kb)):
            arrived(opp, k, p, d, 1)
            share(opp, k, p, 3)

    @pl.when(is_src)
    def _():
        gbuf[0, pl.ds(pl.multiple_of(s0 * blk + (hi * 2 + c) * tb, tb), tb), :] = g_ref[...]
        for k, p in ORDER[PARTS:]:
            own_one(k, p)
        for k, p in ORDER:
            src_near_one(k, p)
        for p in range(PARTS):
            opp_one(0, 1, p)

    @pl.when(not_src)
    def _():
        for k, p in ORDER:
            mid_near_one(k, p)
        for k, p in FIRST:
            mid_far_one(k, p)

    def gather_step(t):
        @pl.when(jnp.logical_and(is_src, t == 3))
        def _():
            for p in range(PARTS):
                opp_one(3, 2, p)

        for when in range(2):
            @pl.when(jnp.logical_and(not_src, t == when))
            def _():
                for p in range(when * PARTS // 2, (when + 1) * PARTS // 2):
                    for k in (3, 2):
                        mid_far_one(k, p)

    def planes_ready(t):
        for when, ks in ((0, (0, 1)), (HALVES, (3, 2))):
            @pl.when(jnp.logical_and(is_src, t == when))
            def _():
                for k in ks:
                    for p in range(PARTS):
                        shared(s0, k, p, 0)
                        for d in range(2):
                            shared(src_near[d], k, p, 1 + d)
                        shared(opp, k, p, 3)

            @pl.when(jnp.logical_and(not_src, t == when))
            def _():
                for k in ks:
                    for p in range(PARTS):
                        for d in range(2):
                            shared(mid_near[d], k, p, 1 + d)
                            shared(mid_far[d], k, p, 3 + d)

    n_items = HALVES + n_ch
    far_slot = lax.rem(x + 2, 4)
    order = (far_slot, xn[0], xn[1], x)

    def group_of(t):
        full = t >= 2 * HALVES
        j = jnp.where(t < HALVES, t, t - HALVES)
        only = jnp.where(t < HALVES, hi, 1 - hi)
        return full, j, only

    def has(h, full, only):
        return jnp.logical_or(full, only == h)

    def rows_of(slot, h, q):
        return pl.ds(pl.multiple_of(slot * blk + (h * 2 + q) * tb, tb), tb)

    def far_copy(j, d, h):
        return rc(cbuf.at[j, rows_of(far_slot, h, d), :], farin.at[d, j, h], fs.at[d, j, h], fr.at[d, j, h], x_dev[d])

    def near_dst(j, d, h, q):
        return nearin.at[d, j, pl.ds((h * 2 + q) * tb, tb), :]

    def direct_copy(j, d, h):
        src = cbuf.at[j, rows_of(xn[d], h, 1 - d), :]
        return rc(src, near_dst(j, d, h, 1 - d), ds.at[d, j, h], dr.at[d, j, h], x_dev[d])

    def relay_copy(j, d, h):
        return rc(relay.at[d, j, h], near_dst(j, d, h, d), rs.at[d, j, h], rr.at[d, j, h], x_dev[d])

    def relay_step(t, _):
        full, j, only = group_of(t)
        for h in range(2):
            @pl.when(has(h, full, only))
            def _():
                for d in range(2):
                    far_copy(j, d, h).wait_recv()
                    relay[d, j, h] = cbuf[j, rows_of(xn[d], h, d), :] + farin[d, j, h]
                    relay_copy(j, d, h).start()

        return 0

    def final_step(t, _):
        full, j, only = group_of(t)
        for h in range(2):
            @pl.when(has(h, full, only))
            def _():
                for d in range(2):
                    direct_copy(j, d, h).wait_recv()
                    relay_copy(j, d, h).wait_recv()
                rows = pl.ds(h * half, half)
                mine = pl.ds(pl.multiple_of(x * blk + h * half, half), half)
                total = cbuf[j, mine, :] + nearin[0, j, rows, :] + nearin[1, j, rows, :]
                o_ref[rows, pl.ds(pl.multiple_of(j * CH, CH), CH)] = total.astype(o_ref.dtype)

        return 0

    def compute_step(t):
        full, j, only = group_of(t)
        paired = sum((t == i).astype(jnp.int32) for i in PAIRS) > 0

        after = sum((t == i + 1).astype(jnp.int32) for i in PAIRS)

        @pl.when(jnp.logical_and(after == 0, jnp.logical_or(full, t < HALVES)))
        def _():
            w_copy(j).wait_recv()

            @pl.when(paired)
            def _():
                w_copy(j + 1).wait_recv()

        def product(rows, wide):
            at = pl.ds(pl.multiple_of(j * CH, CH), wide * CH)
            total = lax.dot_general(gbuf[0, rows, :], w_ref[at, :], NT, preferred_element_type=jnp.float32)
            total += lax.dot_general(gbuf[1, rows, :], wn[at, :], NT, preferred_element_type=jnp.float32)
            for i in range(wide):
                cbuf[j + i, rows, :] = total[:, i * CH : (i + 1) * CH]

        def one(i, _):
            slot = jnp.where(i < 2, jnp.where(i == 0, order[0], order[1]), jnp.where(i == 2, order[2], order[3]))
            for wide in (1, 2):
                this = paired if wide == 2 else jnp.logical_not(paired)

                @pl.when(jnp.logical_and(this, full))
                def _():
                    product(pl.ds(pl.multiple_of(slot * blk, blk), blk), wide)

                @pl.when(jnp.logical_and(this, jnp.logical_not(full)))
                def _():
                    product(pl.ds(pl.multiple_of(slot * blk + only * half, half), half), wide)

            def send(n, _):
                for h in range(2):
                    for d in range(2):
                        @pl.when(jnp.logical_and(has(h, full, only), i == 0))
                        def _():
                            far_copy(j + n, d, h).start()

                        @pl.when(jnp.logical_and(has(h, full, only), i == 1 + d))
                        def _():
                            direct_copy(j + n, d, h).start()

                return 0

            lax.fori_loop(0, jnp.where(paired, 2, 1), send, 0)
            return 0

        @pl.when(after == 0)
        def _():
            lax.fori_loop(0, 4, one, 0)

    def gather_sent():
        def sent(sem):
            rc(own_part(0), own_part(0), sem, sem, partner).wait_send()

        for p in range(PARTS):
            sent(s1s.at[0, p])
            for k in range(4):
                for d in range(2):
                    sent(zs.at[d, 0, k, p])
                    sent(ps.at[1 + d, k, p])
                    if SIDE[k] == d:
                        sent(zs.at[d, 1, k, p])
                sent(ps.at[3, k, p])

        @pl.when(is_src)
        def _():
            for p in range(PARTS):
                for k in range(4):
                    sent(ps.at[0, k, p])
                    sent(zs.at[1 - SIDE[k], 1, k, p])

        @pl.when(not_src)
        def _():
            for p in range(PARTS):
                sent(s1s.at[1, p])
                for k in range(4):
                    sent(ps.at[4, k, p])

    def relayed(t):
        return jnp.clip(t - 2, 0, n_items - 3)

    def finished(t):
        return jnp.where(t >= n_items - 2, n_items - 8, 0)

    def drain(j, _):
        w_copy(j).wait_send()
        for h in range(2):
            for d in range(2):
                far_copy(j, d, h).wait_send()
                direct_copy(j, d, h).wait_send()
                relay_copy(j, d, h).wait_send()
        return 0

    def step(t, _):
        lax.fori_loop(relayed(t - 1), relayed(t), relay_step, 0)
        lax.fori_loop(finished(t - 1), finished(t), final_step, 0)

        planes_ready(t)
        compute_step(t)
        gather_step(t)
        return 0

    lax.fori_loop(0, n_items, step, 0)
    lax.fori_loop(n_items - 3, n_items - 1, relay_step, 0)
    lax.fori_loop(n_items - 8, n_items - 6, final_step, 0)
    lax.fori_loop(n_items - 1, n_items, relay_step, 0)
    gather_sent()
    lax.fori_loop(0, n_ch - 3, drain, 0)
    lax.fori_loop(n_items - 6, n_items, final_step, 0)
    lax.fori_loop(n_ch - 3, n_ch, drain, 0)


def local(grad_out, weight):
    tb, feat = grad_out.shape
    hidden = weight.shape[0]
    n_ch = hidden // CH
    blk = 4 * tb
    dma = pltpu.SemaphoreType.DMA
    vmem = pl.BlockSpec(memory_space=pltpu.VMEM)
    hbm = pl.BlockSpec(memory_space=pltpu.HBM)
    return pl.pallas_call(
        kernel,
        out_shape=jax.ShapeDtypeStruct((blk, hidden), jnp.bfloat16),
        in_specs=[hbm, hbm],
        out_specs=vmem,
        scratch_shapes=[
            pltpu.VMEM((tb, feat), jnp.bfloat16),
            pltpu.VMEM((hidden, feat), jnp.bfloat16),
            pltpu.VMEM((2, 4 * blk, feat), jnp.bfloat16),
            pltpu.VMEM((hidden, feat), jnp.bfloat16),
            pltpu.VMEM((n_ch, 4 * blk, CH), jnp.float32),
            pltpu.VMEM((2, n_ch, 2, tb, CH), jnp.float32),
            pltpu.VMEM((2, n_ch, 2, tb, CH), jnp.float32),
            pltpu.VMEM((2, n_ch, blk, CH), jnp.float32),
            dma((2,)),
            dma((2, PARTS)), dma((3, PARTS)),
            dma((2, 2, 4, PARTS)), dma((2, 2, 4, PARTS)),
            dma((5, 4, PARTS)), dma((5, 4, PARTS)),
            dma((n_ch,)), dma((n_ch,)),
            dma((2, n_ch, 2)), dma((2, n_ch, 2)),
            dma((2, n_ch, 2)), dma((2, n_ch, 2)),
            dma((2, n_ch, 2)), dma((2, n_ch, 2)),
        ],
        compiler_params=pltpu.CompilerParams(
            collective_id=0, has_side_effects=True, vmem_limit_bytes=63 * 1024 * 1024
        ),
    )(grad_out, weight)


def solution(mesh):
    spec = P("col", "row")
    return jax.shard_map(local, mesh=mesh, in_specs=(spec, spec), out_specs=P("row", "col"), check_vma=False)
```

```python
import jax
import jax.numpy as jnp
from jax import lax
from jax.experimental import pallas as pl
from jax.experimental.pallas import tpu as pltpu
from jax.sharding import PartitionSpec as P

MESH = pl.DeviceIdType.MESH
CH = 128
PARTS = 2
FIRST = tuple((k, p) for k in (0, 1) for p in range(PARTS))
ORDER = FIRST + tuple((k, p) for p in range(PARTS) for k in (3, 2))
SIDE = (0, 1, 1, 0)
HALVES = 4
PAIRS = (0, 4, 6, 8)
NT = (((1,), (1,)), ((), ()))


def kernel(
    g_hbm, w_hbm, o_ref, g_ref, w_ref, gbuf, wn, cbuf, relay, farin, nearin,
    ls, s1s, s1r, zs, zr, ps, pr, ws, wr, fs, fr, ds, dr, rs, rr,
):
    n_ch = w_ref.shape[0] // CH
    tb, feat = g_ref.shape
    blk = 4 * tb
    half = blk // 2
    row = lax.axis_index("row")
    col = lax.axis_index("col")
    x = lax.div(row, 2)
    lo = lax.rem(row, 2)
    z = lax.div(col, 4)
    hi = lax.rem(lax.div(col, 2), 2)
    c = lax.rem(col, 2)
    is_src = lax.rem(z, 2) == lo
    not_src = jnp.logical_not(is_src)

    def dev(x=x, lo=lo, z=z, hi=hi, c=c):
        return (x * 2 + lo, z * 4 + hi * 2 + c)

    zn = (lax.rem(z + 1, 8), lax.rem(z + 7, 8))
    xn = (lax.rem(x + 1, 4), lax.rem(x + 3, 4))
    partner = dev(c=1 - c)
    z_dev = (dev(z=zn[0]), dev(z=zn[1]))
    x_dev = (dev(x=xn[0]), dev(x=xn[1]))
    w_dev = dev(lo=1 - lo)
    h_dev = dev(hi=1 - hi)
    wh_dev = dev(lo=1 - lo, hi=1 - hi)

    barrier = pltpu.get_barrier_semaphore()
    peers = (partner, *z_dev, *x_dev, w_dev, h_dev, wh_dev)
    for peer in peers:
        pl.semaphore_signal(barrier, inc=1, device_id=peer, device_id_type=MESH)
    g_in = pltpu.make_async_copy(g_hbm, g_ref, ls.at[0])
    w_in = pltpu.make_async_copy(w_hbm, w_ref, ls.at[1])
    g_in.start()
    w_in.start()
    g_in.wait()
    w_in.wait()
    pl.semaphore_wait(barrier, len(peers))

    def rc(src, dst, ss, sr, to):
        return pltpu.make_async_remote_copy(
            src_ref=src, dst_ref=dst, send_sem=ss, recv_sem=sr, device_id=to, device_id_type=MESH
        )

    piece = tb // PARTS

    def place(slot, l, h, core, p):
        at = pl.multiple_of(slot * blk + (h * 2 + core) * tb + p * piece, piece)
        return gbuf.at[l, pl.ds(at, piece), :]

    def side(k):
        return lax.rem(lax.div(k + 1, 2), 2)

    def block(slot, k, core, p):
        return place(slot, side(k), lax.rem(hi + lax.div(k, 2), 2), core, p)

    def slot_of(shift):
        return lax.div(lax.rem(z + shift, 8), 2)

    s0 = lax.div(z, 2)

    def own_part(p):
        return g_ref.at[pl.ds(p * piece, piece), :]

    @pl.when(is_src)
    def _():
        for p in range(PARTS):
            own = place(s0, 0, hi, c, p)
            for d in range(2):
                rc(own_part(p), own, zs.at[d, 0, 0, p], zr.at[d, 0, 0, p], z_dev[d]).start()
            rc(own_part(p), own, s1s.at[0, p], s1r.at[2, p], h_dev).start()
            rc(own_part(p), own, ps.at[0, 0, p], pr.at[0, 0, p], partner).start()

    @pl.when(not_src)
    def _():
        for p in range(PARTS):
            rc(own_part(p), place(s0, 1, hi, c, p), s1s.at[0, p], s1r.at[0, p], w_dev).start()
        for p in range(PARTS):
            rc(own_part(p), place(s0, 1, hi, c, p), s1s.at[1, p], s1r.at[1, p], wh_dev).start()

    def w_copy(j):
        at = pl.ds(pl.multiple_of(j * CH, CH), CH)
        return rc(w_ref.at[at, :], wn.at[at, :], ws.at[j], wr.at[j], w_dev)

    for j in range(n_ch):
        w_copy(j).start()

    def relay_to(slot, k, p, d, out_r, send_r):
        b = block(slot, k, c, p)
        rc(b, b, zs.at[d, send_r, k, p], zr.at[d, out_r, k, p], z_dev[d]).start()

    def share(slot, k, p, i):
        b = block(slot, k, c, p)
        rc(b, b, ps.at[i, k, p], pr.at[i, k, p], partner).start()

    def arrived(slot, k, p, d, r):
        b = block(slot, k, c, p)
        rc(b, b, zs.at[d, r, k, p], zr.at[d, r, k, p], z_dev[d]).wait_recv()

    def shared(slot, k, p, i):
        b = block(slot, k, 1 - c, p)
        rc(b, b, ps.at[i, k, p], pr.at[i, k, p], partner).wait_recv()

    def first_of(k, p):
        b = block(s0, k, c, p)
        rc(b, b, s1s.at[0, p], s1r.at[k - 1, p], h_dev).wait_recv()

    src_near = (slot_of(6), slot_of(2))
    opp = slot_of(4)
    mid_near = (slot_of(7), slot_of(1))
    mid_far = (slot_of(5), slot_of(3))
    early = (jnp.where(is_src, s0, mid_near[0]), jnp.where(is_src, src_near[1], mid_near[1]))
    late = (jnp.where(is_src, src_near[0], mid_far[0]), jnp.where(is_src, opp, mid_far[1]))

    def src_near_one(k, p):
        for d in range(2):
            arrived(src_near[d], k, p, d, 0)
            relay_to(src_near[d], k, p, d, 1, 1)
            share(src_near[d], k, p, 1 + d)

    def mid_near_one(k, p):
        for d in range(2):
            arrived(mid_near[d], k, p, d, 0)
            relay_to(mid_near[d], k, p, d, 0, 0)
            share(mid_near[d], k, p, 1 + d)

    def own_one(k, p):
        first_of(k, p)
        for d in range(2):
            relay_to(s0, k, p, d, 0, 0)
        share(s0, k, p, 0)

    def mid_far_one(k, p):
        for d in range(2):
            arrived(mid_far[d], k, p, d, 1)

            @pl.when(side(k) == d)
            def _():
                relay_to(mid_far[d], k, p, d, 1, 1)

            share(mid_far[d], k, p, 3 + d)

    def opp_one(ka, kb, p):
        for d, k in ((0, ka), (1, kb)):
            arrived(opp, k, p, d, 1)
            share(opp, k, p, 3)

    @pl.when(is_src)
    def _():
        gbuf[0, pl.ds(pl.multiple_of(s0 * blk + (hi * 2 + c) * tb, tb), tb), :] = g_ref[...]
        for k, p in ORDER[PARTS:]:
            own_one(k, p)
        for k, p in ORDER:
            src_near_one(k, p)
        for p in range(PARTS):
            opp_one(0, 1, p)

    @pl.when(not_src)
    def _():
        for k, p in ORDER:
            mid_near_one(k, p)
        for k, p in FIRST:
            mid_far_one(k, p)

    def gather_step(t):
        @pl.when(jnp.logical_and(is_src, t == 3))
        def _():
            for p in range(PARTS):
                opp_one(3, 2, p)

        for when in range(2):
            @pl.when(jnp.logical_and(not_src, t == when))
            def _():
                for p in range(when * PARTS // 2, (when + 1) * PARTS // 2):
                    for k in (3, 2):
                        mid_far_one(k, p)

    def planes_ready(t):
        for when, ks in ((0, (0, 1)), (HALVES, (3, 2))):
            @pl.when(jnp.logical_and(is_src, t == when))
            def _():
                for k in ks:
                    for p in range(PARTS):
                        shared(s0, k, p, 0)
                        for d in range(2):
                            shared(src_near[d], k, p, 1 + d)
                        shared(opp, k, p, 3)

            @pl.when(jnp.logical_and(not_src, t == when))
            def _():
                for k in ks:
                    for p in range(PARTS):
                        for d in range(2):
                            shared(mid_near[d], k, p, 1 + d)
                            shared(mid_far[d], k, p, 3 + d)

    n_items = HALVES + n_ch
    far_slot = lax.rem(x + 2, 4)
    order = (far_slot, xn[0], xn[1], x)

    def group_of(t):
        full = t >= 2 * HALVES
        j = jnp.where(t < HALVES, t, t - HALVES)
        only = jnp.where(t < HALVES, hi, 1 - hi)
        return full, j, only

    def has(h, full, only):
        return jnp.logical_or(full, only == h)

    def rows_of(slot, h, q):
        return pl.ds(pl.multiple_of(slot * blk + (h * 2 + q) * tb, tb), tb)

    def far_copy(j, d, h):
        return rc(cbuf.at[j, rows_of(far_slot, h, d), :], farin.at[d, j, h], fs.at[d, j, h], fr.at[d, j, h], x_dev[d])

    def near_dst(j, d, h, q):
        return nearin.at[d, j, pl.ds((h * 2 + q) * tb, tb), :]

    def direct_copy(j, d, h):
        src = cbuf.at[j, rows_of(xn[d], h, 1 - d), :]
        return rc(src, near_dst(j, d, h, 1 - d), ds.at[d, j, h], dr.at[d, j, h], x_dev[d])

    def relay_copy(j, d, h):
        return rc(relay.at[d, j, h], near_dst(j, d, h, d), rs.at[d, j, h], rr.at[d, j, h], x_dev[d])

    def relay_step(t, _):
        full, j, only = group_of(t)
        for h in range(2):
            @pl.when(has(h, full, only))
            def _():
                for d in range(2):
                    far_copy(j, d, h).wait_recv()
                    relay[d, j, h] = cbuf[j, rows_of(xn[d], h, d), :] + farin[d, j, h]
                    relay_copy(j, d, h).start()

        return 0

    def final_step(t, _):
        full, j, only = group_of(t)
        for h in range(2):
            @pl.when(has(h, full, only))
            def _():
                for d in range(2):
                    direct_copy(j, d, h).wait_recv()
                    relay_copy(j, d, h).wait_recv()
                rows = pl.ds(h * half, half)
                mine = pl.ds(pl.multiple_of(x * blk + h * half, half), half)
                total = cbuf[j, mine, :] + nearin[0, j, rows, :] + nearin[1, j, rows, :]
                o_ref[rows, pl.ds(pl.multiple_of(j * CH, CH), CH)] = total.astype(o_ref.dtype)

        return 0

    def compute_step(t):
        full, j, only = group_of(t)
        paired = sum((t == i).astype(jnp.int32) for i in PAIRS) > 0

        after = sum((t == i + 1).astype(jnp.int32) for i in PAIRS)

        @pl.when(jnp.logical_and(after == 0, jnp.logical_or(full, t < HALVES)))
        def _():
            w_copy(j).wait_recv()

            @pl.when(paired)
            def _():
                w_copy(j + 1).wait_recv()

        def product(rows, wide):
            at = pl.ds(pl.multiple_of(j * CH, CH), wide * CH)
            total = lax.dot_general(gbuf[0, rows, :], w_ref[at, :], NT, preferred_element_type=jnp.float32)
            total += lax.dot_general(gbuf[1, rows, :], wn[at, :], NT, preferred_element_type=jnp.float32)
            for i in range(wide):
                cbuf[j + i, rows, :] = total[:, i * CH : (i + 1) * CH]

        def one(i, _):
            slot = jnp.where(i < 2, jnp.where(i == 0, order[0], order[1]), jnp.where(i == 2, order[2], order[3]))
            for wide in (1, 2):
                this = paired if wide == 2 else jnp.logical_not(paired)

                @pl.when(jnp.logical_and(this, full))
                def _():
                    product(pl.ds(pl.multiple_of(slot * blk, blk), blk), wide)

                @pl.when(jnp.logical_and(this, jnp.logical_not(full)))
                def _():
                    product(pl.ds(pl.multiple_of(slot * blk + only * half, half), half), wide)

            def send(n, _):
                for h in range(2):
                    for d in range(2):
                        @pl.when(jnp.logical_and(has(h, full, only), i == 0))
                        def _():
                            far_copy(j + n, d, h).start()

                        @pl.when(jnp.logical_and(has(h, full, only), i == 1 + d))
                        def _():
                            direct_copy(j + n, d, h).start()

                return 0

            lax.fori_loop(0, jnp.where(paired, 2, 1), send, 0)
            return 0

        @pl.when(after == 0)
        def _():
            lax.fori_loop(0, 4, one, 0)

    def gather_sent():
        def sent(sem):
            rc(own_part(0), own_part(0), sem, sem, partner).wait_send()

        for p in range(PARTS):
            sent(s1s.at[0, p])
            for k in range(4):
                for d in range(2):
                    sent(zs.at[d, 0, k, p])
                    sent(ps.at[1 + d, k, p])
                    if SIDE[k] == d:
                        sent(zs.at[d, 1, k, p])
                sent(ps.at[3, k, p])

        @pl.when(is_src)
        def _():
            for p in range(PARTS):
                for k in range(4):
                    sent(ps.at[0, k, p])
                    sent(zs.at[1 - SIDE[k], 1, k, p])

        @pl.when(not_src)
        def _():
            for p in range(PARTS):
                sent(s1s.at[1, p])
                for k in range(4):
                    sent(ps.at[4, k, p])

    def relayed(t):
        return jnp.clip(t - 2, 0, n_items - 3)

    def finished(t):
        return jnp.where(t >= n_items - 2, n_items - 8, 0)

    def drain(j, _):
        w_copy(j).wait_send()
        for h in range(2):
            for d in range(2):
                far_copy(j, d, h).wait_send()
                direct_copy(j, d, h).wait_send()
                relay_copy(j, d, h).wait_send()
        return 0

    def step(t, _):
        lax.fori_loop(relayed(t - 1), relayed(t), relay_step, 0)
        lax.fori_loop(finished(t - 1), finished(t), final_step, 0)

        planes_ready(t)
        compute_step(t)
        gather_step(t)
        return 0

    lax.fori_loop(0, n_items, step, 0)
    lax.fori_loop(n_items - 3, n_items - 1, relay_step, 0)
    lax.fori_loop(n_items - 8, n_items - 6, final_step, 0)
    lax.fori_loop(n_items - 1, n_items, relay_step, 0)
    gather_sent()
    lax.fori_loop(0, n_ch - 3, drain, 0)
    lax.fori_loop(n_items - 6, n_items, final_step, 0)
    lax.fori_loop(n_ch - 3, n_ch, drain, 0)


def local(grad_out, weight):
    tb, feat = grad_out.shape
    hidden = weight.shape[0]
    n_ch = hidden // CH
    blk = 4 * tb
    dma = pltpu.SemaphoreType.DMA
    vmem = pl.BlockSpec(memory_space=pltpu.VMEM)
    hbm = pl.BlockSpec(memory_space=pltpu.HBM)
    return pl.pallas_call(
        kernel,
        out_shape=jax.ShapeDtypeStruct((blk, hidden), jnp.bfloat16),
        in_specs=[hbm, hbm],
        out_specs=vmem,
        scratch_shapes=[
            pltpu.VMEM((tb, feat), jnp.bfloat16),
            pltpu.VMEM((hidden, feat), jnp.bfloat16),
            pltpu.VMEM((2, 4 * blk, feat), jnp.bfloat16),
            pltpu.VMEM((hidden, feat), jnp.bfloat16),
            pltpu.VMEM((n_ch, 4 * blk, CH), jnp.float32),
            pltpu.VMEM((2, n_ch, 2, tb, CH), jnp.float32),
            pltpu.VMEM((2, n_ch, 2, tb, CH), jnp.float32),
            pltpu.VMEM((2, n_ch, blk, CH), jnp.float32),
            dma((2,)),
            dma((2, PARTS)), dma((3, PARTS)),
            dma((2, 2, 4, PARTS)), dma((2, 2, 4, PARTS)),
            dma((5, 4, PARTS)), dma((5, 4, PARTS)),
            dma((n_ch,)), dma((n_ch,)),
            dma((2, n_ch, 2)), dma((2, n_ch, 2)),
            dma((2, n_ch, 2)), dma((2, n_ch, 2)),
            dma((2, n_ch, 2)), dma((2, n_ch, 2)),
        ],
        compiler_params=pltpu.CompilerParams(
            collective_id=0, has_side_effects=True, vmem_limit_bytes=63 * 1024 * 1024
        ),
    )(grad_out, weight)


def solution(mesh):
    spec = P("col", "row")
    return jax.shard_map(local, mesh=mesh, in_specs=(spec, spec), out_specs=P("row", "col"), check_vma=False)
```
